8 devices in a mesh: dp: 1 (over z), tp: 2 (over y), sp: 4 (over x, core).
Axes of the slice: x: 2, y: 2, z: 1, core: 2. Of those that a mesh axis runs over, the one named last changes fastest.
Arguments:
- x_in: bfloat16 [512, 2304], P('dp')
- cur_pos: int32 [512], P('dp')
- w_pre: float32 [2304], replicated
- w_q: bfloat16 [2304, 2048], P(None, 'tp')
- w_k: bfloat16 [2304, 1024], P(None, 'tp')
- w_v: bfloat16 [2304, 1024], P(None, 'tp')
- w_o: bfloat16 [2048, 2304], P('tp')
- w_post: float32 [2304], replicated
- k_cache: bfloat16 [512, 256, 4, 256], P('dp', 'sp', 'tp')
- v_cache: bfloat16 [512, 256, 4, 256], P('dp', 'sp', 'tp')
Outputs:
- output 1: bfloat16 [512, 2304], P('dp')
- output 2: bfloat16 [512, 256, 4, 256], P('dp', 'sp', 'tp')
- output 3: bfloat16 [512, 256, 4, 256], P('dp', 'sp', 'tp')
All inputs are finite; a program needn't handle non-finite values.
Results may differ from the reference program's by a relative error of at most 0.00629532.
Values sent between devices are 32-bit elements.
A program may use at most 1 GiB of HBM per device.

```python
import jax
import jax.numpy as jnp
from jax import lax

BATCH_SIZE = 512
SEQ_LEN = 256
D_MODEL = 2304
NUM_HEADS = 8
KV_HEADS = 4
HEAD_DIM = 256
HOT_KEYS = 48

SOFT_CAP = 50.0
ROPE_BASE = 10000.0
NORM_EPS = 1e-6


def rms_scale(tensor, gain_w):
    mean_sq = jnp.mean(tensor * tensor, axis=-1, keepdims=True)
    return tensor * lax.rsqrt(mean_sq + NORM_EPS) * (1.0 + gain_w)


def rotary(tensor, positions):
    half_dim = tensor.shape[-1] // 2
    inv_freq = ROPE_BASE ** (-2.0 * jnp.arange(half_dim, dtype=jnp.float32) / (2 * half_dim))
    angles = positions.astype(jnp.float32)[:, None] * inv_freq[None, :]
    angles = angles.reshape((angles.shape[0],) + (1,) * (tensor.ndim - 2) + (half_dim,))
    cos_tab = jnp.cos(angles)
    sin_tab = jnp.sin(angles)
    lo_half = tensor[..., :half_dim]
    hi_half = tensor[..., half_dim:]
    return jnp.concatenate([lo_half * cos_tab - hi_half * sin_tab, hi_half * cos_tab + lo_half * sin_tab], axis=-1)


def setup_inputs(seed: int = 0, part: int = 0) -> dict:
    part_keys = jax.random.split(jax.random.fold_in(jax.random.key(seed), part), 6)
    shared_keys = jax.random.split(jax.random.key(seed + 1), 7)
    q_cols = NUM_HEADS * HEAD_DIM
    kv_cols = KV_HEADS * HEAD_DIM
    cache_shape = (BATCH_SIZE, SEQ_LEN, KV_HEADS, HEAD_DIM)
    x_in = jax.random.normal(part_keys[0], (BATCH_SIZE, D_MODEL), jnp.float32).astype(jnp.bfloat16)
    drawn_pos = jax.random.randint(part_keys[1], (BATCH_SIZE,), 0, SEQ_LEN)
    long_row = jax.random.randint(part_keys[2], (), 0, BATCH_SIZE)
    cur_pos = jnp.where(jnp.arange(BATCH_SIZE) == long_row, SEQ_LEN - 1, drawn_pos).astype(jnp.int32)
    hot_mark = jax.random.randint(part_keys[3], (BATCH_SIZE, SEQ_LEN, KV_HEADS, 1), 0, SEQ_LEN) < HOT_KEYS
    key_scale = jnp.where(hot_mark, 2.5, 0.03)
    k_cache = (jax.random.normal(part_keys[4], cache_shape, jnp.float32) * key_scale).astype(jnp.bfloat16)
    v_cache = jax.random.normal(part_keys[5], cache_shape, jnp.float32).astype(jnp.bfloat16)
    w_pre = 0.5 * jax.random.normal(shared_keys[0], (D_MODEL,), jnp.float32)
    w_q = (jax.random.normal(shared_keys[1], (D_MODEL, q_cols), jnp.float32) * (36.0 * D_MODEL ** -0.5)).astype(jnp.bfloat16)
    w_k = (jax.random.normal(shared_keys[2], (D_MODEL, kv_cols), jnp.float32) * (2.2 * D_MODEL ** -0.5)).astype(jnp.bfloat16)
    w_v = (jax.random.normal(shared_keys[3], (D_MODEL, kv_cols), jnp.float32) * D_MODEL ** -0.5).astype(jnp.bfloat16)
    w_o = (jax.random.normal(shared_keys[4], (q_cols, D_MODEL), jnp.float32) * q_cols ** -0.5).astype(jnp.bfloat16)
    w_post = 0.5 * jax.random.normal(shared_keys[5], (D_MODEL,), jnp.float32)
    return {'x_in': x_in, 'cur_pos': cur_pos, 'w_pre': w_pre, 'w_q': w_q, 'w_k': w_k, 'w_v': w_v, 'w_o': w_o, 'w_post': w_post, 'k_cache': k_cache, 'v_cache': v_cache}


def reference(x_in, cur_pos, w_pre, w_q, w_k, w_v, w_o, w_post, k_cache, v_cache):
    group_size = NUM_HEADS // KV_HEADS
    seq_ids = jnp.arange(SEQ_LEN)
    normed = rms_scale(x_in.astype(jnp.float32), w_pre).astype(jnp.bfloat16)
    q_proj = jnp.dot(normed, w_q, preferred_element_type=jnp.float32).reshape(BATCH_SIZE, NUM_HEADS, HEAD_DIM)
    k_proj = jnp.dot(normed, w_k, preferred_element_type=jnp.float32).reshape(BATCH_SIZE, KV_HEADS, HEAD_DIM)
    q_rot = rotary(q_proj, cur_pos).astype(jnp.bfloat16)
    k_new = rotary(k_proj, cur_pos).astype(jnp.bfloat16)
    v_new = jnp.dot(normed, w_v, preferred_element_type=jnp.float32).reshape(BATCH_SIZE, KV_HEADS, HEAD_DIM).astype(jnp.bfloat16)
    slot_hit = (seq_ids[None, :] == cur_pos[:, None])[:, :, None, None]
    k_out = jnp.where(slot_hit, k_new[:, None], k_cache)
    v_out = jnp.where(slot_hit, v_new[:, None], v_cache)

    def one_row(row_data):
        q_row, k_row, v_row, pos_row = row_data
        q_grp = q_row.astype(jnp.float32).reshape(KV_HEADS, group_size, HEAD_DIM)
        raw_score = jnp.einsum('grd,tgd->grt', q_grp, k_row.astype(jnp.float32)) * HEAD_DIM ** -0.5
        capped = SOFT_CAP * jnp.tanh(raw_score / SOFT_CAP)
        capped = jnp.where(seq_ids <= pos_row, capped, -jnp.inf)
        prob_w = jax.nn.softmax(capped, axis=-1)
        attn_row = jnp.einsum('grt,tgd->grd', prob_w, v_row.astype(jnp.float32))
        return attn_row.reshape(NUM_HEADS * HEAD_DIM)

    attn_out = lax.map(one_row, (q_rot, k_out, v_out, cur_pos))
    proj_sum = jnp.dot(attn_out.astype(jnp.bfloat16), w_o, preferred_element_type=jnp.float32)
    x_out = (x_in.astype(jnp.float32) + rms_scale(proj_sum, w_post)).astype(jnp.bfloat16)
    return (x_out, k_out, v_out)
```

```python
import functools

import jax
import jax.numpy as jnp
from jax import lax
from jax.experimental import pallas as pl
from jax.experimental.pallas import tpu as pltpu
from jax.sharding import PartitionSpec as P

SOFT_CAP = 50.0
ROPE_BASE = 10000.0
NORM_EPS = 1e-6
NEG_FILL = -1e30
F32 = jnp.float32
BF16 = jnp.bfloat16


def rms_scale(tensor, gain_w):
    mean_sq = jnp.mean(tensor * tensor, axis=-1, keepdims=True)
    return tensor * lax.rsqrt(mean_sq + NORM_EPS) * (1.0 + gain_w)


def stream_kernel(cfg, pos_s, x_hbm, gain, cos_t, sin_t, wq_hbm, wk_hbm, wv_hbm, kc, vc, k_out, v_out, o_ref, lse_ref,
                  x_v, a_v, wq_v, wk_v, wv_v, q_s, kn_s, vn_s, kbuf, vbuf, p_s,
                  w_sem, kin, vin, kout, vout):
    rows, seq, kv, hd, blk, nbuf, lag = cfg
    nblk = rows // blk
    groups = blk // 2
    base = lax.axis_index('sp') * seq

    def k_in(j, s):
        return pltpu.make_async_copy(kc.at[pl.ds(j * blk, blk)], kbuf.at[s], kin.at[s])

    def v_in(j, s):
        return pltpu.make_async_copy(vc.at[pl.ds(j * blk, blk)], vbuf.at[s], vin.at[s])

    def k_o(j, s):
        return pltpu.make_async_copy(kbuf.at[s], k_out.at[pl.ds(j * blk, blk)], kout.at[s])

    def v_o(j, s):
        return pltpu.make_async_copy(vbuf.at[s], v_out.at[pl.ds(j * blk, blk)], vout.at[s])

    loads = [pltpu.make_async_copy(x_hbm, x_v, w_sem.at[0]), pltpu.make_async_copy(wq_hbm, wq_v, w_sem.at[1]),
             pltpu.make_async_copy(wk_hbm, wk_v, w_sem.at[2]), pltpu.make_async_copy(wv_hbm, wv_v, w_sem.at[3])]
    for c in loads:
        c.start()
    for s in range(nbuf):
        k_in(s, s).start()
        v_in(s, s).start()

    loads[0].wait()
    step = 32

    @pl.loop(0, rows // step)
    def _(i):
        r = pl.ds(pl.multiple_of(i * step, step), step)
        a_v[r, :] = rms_scale(x_v[r, :].astype(F32), gain[...]).astype(BF16)

    half = hd // 2
    nq = wq_v.shape[1] // hd

    def rope_store(acc, dst, h, stride):
        lo, hi = acc[:, :half], acc[:, half:]
        c, s = cos_t[...], sin_t[...]
        r_lo = (lo * c - hi * s).astype(BF16).astype(F32)
        r_hi = (hi * c + lo * s).astype(BF16).astype(F32)
        idx = pl.ds(h, rows, stride=stride)
        dst[0, idx, :] = r_lo
        dst[1, idx, :] = r_hi

    loads[1].wait()
    for h in range(nq):
        acc = jnp.dot(a_v[...], wq_v[:, h * hd:(h + 1) * hd], preferred_element_type=F32)
        rope_store(acc, q_s, h, nq)
    loads[2].wait()
    for h in range(kv):
        acc = jnp.dot(a_v[...], wk_v[:, h * hd:(h + 1) * hd], preferred_element_type=F32)
        rope_store(acc, kn_s, h, kv)
    loads[3].wait()
    for h in range(kv):
        acc = jnp.dot(a_v[...], wv_v[:, h * hd:(h + 1) * hd], preferred_element_type=F32)
        acc = acc.astype(BF16).astype(F32)
        idx = pl.ds(h, rows, stride=kv)
        vn_s[0, idx, :] = acc[:, :half]
        vn_s[1, idx, :] = acc[:, half:]

    ng = nq * 2
    width = 2 * seq * kv
    ri = lax.broadcasted_iota(jnp.int32, (ng, width), 0)
    ci = lax.broadcasted_iota(jnp.int32, (ng, width), 1)
    first = ri < nq
    same = jnp.logical_and(ri // nq == ci // (seq * kv), (ri % nq) // (nq // kv) == ci % kv)
    t_id = jnp.where(same, (ci % (seq * kv)) // kv + base, 1 << 20)
    scale = hd ** -0.5 / SOFT_CAP

    @pl.loop(0, nblk)
    def _(j):
        slot = lax.rem(j, nbuf)

        @pl.when(jnp.logical_and(j >= lag, j + nbuf - lag < nblk))
        def _():
            s2 = lax.rem(j - lag, nbuf)
            k_o(j - lag, s2).wait()
            k_in(j - lag + nbuf, s2).start()
            v_o(j - lag, s2).wait()
            v_in(j - lag + nbuf, s2).start()

        k_in(j, slot).wait()
        v_in(j, slot).wait()
        for i in range(blk):
            b = j * blk + i
            t = pos_s[b] - base
            hit = jnp.logical_and(t >= 0, t < seq)
            tt = jnp.clip(t, 0, seq - 1)
            r = pl.ds(kv * b, kv)
            for buf, new in ((kbuf, kn_s), (vbuf, vn_s)):
                row = jnp.concatenate([new[0, r, :], new[1, r, :]], axis=-1)
                old = buf[slot, i, tt].astype(F32)
                buf[slot, i, tt] = jnp.where(hit, row, old).astype(BF16)

        parts = []
        for g in range(groups):
            r = pl.ds(pl.multiple_of((j * groups + g) * ng, ng), ng)
            qg = jnp.concatenate([q_s[0, r, :], q_s[1, r, :]], axis=-1).astype(BF16)
            km = kbuf[slot, 2 * g:2 * g + 2].reshape(width, hd)
            s = lax.dot_general(qg, km, (((1,), (1,)), ((), ())), preferred_element_type=F32)
            s = SOFT_CAP * jnp.tanh(s * scale)
            b = j * blk + 2 * g
            lim = jnp.where(first, pos_s[b], pos_s[b + 1])
            parts.append(jnp.where(t_id <= lim, s, NEG_FILL))
        sc = jnp.concatenate(parts, axis=0)
        m = jnp.max(sc, axis=-1, keepdims=True)
        e = jnp.where(sc > 0.5 * NEG_FILL, jnp.exp(sc - m), 0.0)
        l = jnp.sum(e, axis=-1, keepdims=True)
        some = l > 0.0
        inv = jnp.where(some, 1.0 / jnp.where(some, l, 1.0), 0.0)
        p_s[...] = e.astype(BF16)
        for g in range(groups):
            vm = vbuf[slot, 2 * g:2 * g + 2].reshape(width, hd)
            o = jnp.dot(p_s[g * ng:(g + 1) * ng, :], vm, preferred_element_type=F32)
            o_ref[pl.ds(pl.multiple_of((j * groups + g) * ng, ng), ng), :] = o * inv[g * ng:(g + 1) * ng, :]
        lse = jnp.where(some, m + jnp.log(jnp.where(some, l, 1.0)), NEG_FILL)
        lse_t = jnp.broadcast_to(lse, (groups * ng, 128)).T
        lse_ref[pl.ds(j, 1), :] = lse_t[0:1, :]
        k_o(j, slot).start()
        v_o(j, slot).start()

    for i in range(nbuf):
        j = nblk - nbuf + i
        k_o(j, j % nbuf).wait()
        v_o(j, j % nbuf).wait()


def solution(mesh):
    cache_spec = P('dp', 'sp', 'tp', None)

    def local_step(x_in, cur_pos, w_pre, w_q, w_k, w_v, w_o, w_post, k_cache, v_cache):
        rows, seq, kv, hd = k_cache.shape
        d_model = x_in.shape[1]
        nq = w_q.shape[1] // hd
        half = hd // 2
        blk, nbuf, lag = 32, 8, 3
        nblk = rows // blk
        inv_freq = ROPE_BASE ** (-2.0 * jnp.arange(half, dtype=F32) / hd)
        ang = cur_pos.astype(F32)[:, None] * inv_freq[None, :]
        cos_t, sin_t = jnp.cos(ang), jnp.sin(ang)
        vmem, hbm = pl.BlockSpec(memory_space=pltpu.VMEM), pl.BlockSpec(memory_space=pl.ANY)
        dma = pltpu.SemaphoreType.DMA
        cfg = (rows, seq, kv, hd, blk, nbuf, lag)
        k_out, v_out, o_part, lse = pl.pallas_call(
            functools.partial(stream_kernel, cfg),
            name='stream',
            out_shape=[jax.ShapeDtypeStruct(k_cache.shape, BF16), jax.ShapeDtypeStruct(v_cache.shape, BF16),
                       jax.ShapeDtypeStruct((rows * nq, hd), F32), jax.ShapeDtypeStruct((nblk, blk * nq), F32)],
            in_specs=[pl.BlockSpec(memory_space=pltpu.SMEM), hbm, vmem, vmem, vmem, hbm, hbm, hbm, hbm, hbm],
            out_specs=[hbm, hbm, vmem, vmem],
            scratch_shapes=[
                pltpu.VMEM((rows, d_model), BF16), pltpu.VMEM((rows, d_model), BF16),
                pltpu.VMEM(w_q.shape, BF16), pltpu.VMEM(w_k.shape, BF16), pltpu.VMEM(w_v.shape, BF16),
                pltpu.VMEM((2, rows * nq, half), F32), pltpu.VMEM((2, rows * kv, half), F32), pltpu.VMEM((2, rows * kv, half), F32),
                pltpu.VMEM((nbuf, blk, seq, kv, hd), BF16), pltpu.VMEM((nbuf, blk, seq, kv, hd), BF16),
                pltpu.VMEM((blk * nq, 2 * seq * kv), BF16),
                dma((4,)), dma((nbuf,)), dma((nbuf,)), dma((nbuf,)), dma((nbuf,))],
            compiler_params=pltpu.CompilerParams(vmem_limit_bytes=66_000_000),
            cost_estimate=pl.CostEstimate(flops=10 ** 10, bytes_accessed=150_000_000, transcendentals=0),
        )(cur_pos, x_in, w_pre[None, :], cos_t, sin_t, w_q, w_k, w_v, k_cache, v_cache)

        block_out = o_part.reshape(rows, nq, hd)
        lse = lse.reshape(rows, nq)
        top = lax.pmax(lse, 'sp')
        weight = jnp.exp(lse - top)
        packed = jnp.concatenate([block_out * weight[..., None], weight[..., None]], axis=-1)
        merged = lax.psum(packed, 'sp')
        attn_out = (merged[..., :hd] / merged[..., hd:]).reshape(rows, nq * hd)
        proj_part = jnp.dot(attn_out.astype(BF16), w_o, preferred_element_type=F32)
        proj_sum = lax.psum(proj_part, 'tp')
        x_out = (x_in.astype(F32) + rms_scale(proj_sum, w_post)).astype(BF16)
        return x_out, k_out, v_out

    return jax.shard_map(local_step, mesh=mesh,
                         in_specs=(P('dp', None), P('dp'), P(None), P(None, 'tp'), P(None, 'tp'), P(None, 'tp'), P('tp', None), P(None), cache_spec, cache_spec),
                         out_specs=(P('dp', None), cache_spec, cache_spec), check_vma=False)
```

```python
import functools

import jax
import jax.numpy as jnp
from jax import lax
from jax.experimental import pallas as pl
from jax.experimental.pallas import tpu as pltpu
from jax.sharding import PartitionSpec as P

SOFT_CAP = 50.0
ROPE_BASE = 10000.0
NORM_EPS = 1e-6
NEG_FILL = -1e30
F32 = jnp.float32
BF16 = jnp.bfloat16


def rms_scale(tensor, gain_w):
    mean_sq = jnp.mean(tensor * tensor, axis=-1, keepdims=True)
    return tensor * lax.rsqrt(mean_sq + NORM_EPS) * (1.0 + gain_w)


def stream_kernel(cfg, pos_s, x_hbm, gain, cos_t, sin_t, wq_hbm, wk_hbm, wv_hbm, kc, vc, k_out, v_out, o_ref, lse_ref,
                  x_v, a_v, wq_v, wk_v, wv_v, q_s, kn_s, vn_s, kbuf, vbuf, p_s,
                  w_sem, kin, vin, kout, vout):
    rows, seq, kv, hd, blk, nbuf, lag = cfg
    nblk = rows // blk
    groups = blk // 2
    base = lax.axis_index('sp') * seq

    def k_in(j, s):
        return pltpu.make_async_copy(kc.at[pl.ds(j * blk, blk)], kbuf.at[s], kin.at[s])

    def v_in(j, s):
        return pltpu.make_async_copy(vc.at[pl.ds(j * blk, blk)], vbuf.at[s], vin.at[s])

    def k_o(j, s):
        return pltpu.make_async_copy(kbuf.at[s], k_out.at[pl.ds(j * blk, blk)], kout.at[s])

    def v_o(j, s):
        return pltpu.make_async_copy(vbuf.at[s], v_out.at[pl.ds(j * blk, blk)], vout.at[s])

    loads = [pltpu.make_async_copy(x_hbm, x_v, w_sem.at[0]), pltpu.make_async_copy(wq_hbm, wq_v, w_sem.at[1]),
             pltpu.make_async_copy(wk_hbm, wk_v, w_sem.at[2]), pltpu.make_async_copy(wv_hbm, wv_v, w_sem.at[3])]
    for c in loads:
        c.start()
    for s in range(nbuf):
        k_in(s, s).start()
        v_in(s, s).start()

    loads[0].wait()
    step = 32

    @pl.loop(0, rows // step)
    def _(i):
        r = pl.ds(pl.multiple_of(i * step, step), step)
        a_v[r, :] = rms_scale(x_v[r, :].astype(F32), gain[...]).astype(BF16)

    half = hd // 2
    nq = wq_v.shape[1] // hd

    def rope_store(acc, dst, h, stride):
        lo, hi = acc[:, :half], acc[:, half:]
        c, s = cos_t[...], sin_t[...]
        r_lo = (lo * c - hi * s).astype(BF16).astype(F32)
        r_hi = (hi * c + lo * s).astype(BF16).astype(F32)
        idx = pl.ds(h, rows, stride=stride)
        dst[0, idx, :] = r_lo
        dst[1, idx, :] = r_hi

    loads[1].wait()
    for h in range(nq):
        acc = jnp.dot(a_v[...], wq_v[:, h * hd:(h + 1) * hd], preferred_element_type=F32)
        rope_store(acc, q_s, h, nq)
    loads[2].wait()
    for h in range(kv):
        acc = jnp.dot(a_v[...], wk_v[:, h * hd:(h + 1) * hd], preferred_element_type=F32)
        rope_store(acc, kn_s, h, kv)
    loads[3].wait()
    for h in range(kv):
        acc = jnp.dot(a_v[...], wv_v[:, h * hd:(h + 1) * hd], preferred_element_type=F32)
        acc = acc.astype(BF16).astype(F32)
        idx = pl.ds(h, rows, stride=kv)
        vn_s[0, idx, :] = acc[:, :half]
        vn_s[1, idx, :] = acc[:, half:]

    ng = nq * 2
    width = 2 * seq * kv
    ri = lax.broadcasted_iota(jnp.int32, (ng, width), 0)
    ci = lax.broadcasted_iota(jnp.int32, (ng, width), 1)
    first = ri < nq
    same = jnp.logical_and(ri // nq == ci // (seq * kv), (ri % nq) // (nq // kv) == ci % kv)
    t_id = jnp.where(same, (ci % (seq * kv)) // kv + base, 1 << 20)
    scale = hd ** -0.5 / SOFT_CAP

    @pl.loop(0, nblk)
    def _(j):
        slot = lax.rem(j, nbuf)

        @pl.when(jnp.logical_and(j >= lag, j + nbuf - lag < nblk))
        def _():
            s2 = lax.rem(j - lag, nbuf)
            k_o(j - lag, s2).wait()
            k_in(j - lag + nbuf, s2).start()
            v_o(j - lag, s2).wait()
            v_in(j - lag + nbuf, s2).start()

        k_in(j, slot).wait()
        v_in(j, slot).wait()
        for i in range(blk):
            b = j * blk + i
            t = pos_s[b] - base
            hit = jnp.logical_and(t >= 0, t < seq)
            tt = jnp.clip(t, 0, seq - 1)
            r = pl.ds(kv * b, kv)
            for buf, new in ((kbuf, kn_s), (vbuf, vn_s)):
                row = jnp.concatenate([new[0, r, :], new[1, r, :]], axis=-1)
                old = buf[slot, i, tt].astype(F32)
                buf[slot, i, tt] = jnp.where(hit, row, old).astype(BF16)

        parts = []
        for g in range(groups):
            r = pl.ds(pl.multiple_of((j * groups + g) * ng, ng), ng)
            qg = jnp.concatenate([q_s[0, r, :], q_s[1, r, :]], axis=-1).astype(BF16)
            km = kbuf[slot, 2 * g:2 * g + 2].reshape(width, hd)
            s = lax.dot_general(qg, km, (((1,), (1,)), ((), ())), preferred_element_type=F32)
            s = SOFT_CAP * jnp.tanh(s * scale)
            b = j * blk + 2 * g
            lim = jnp.where(first, pos_s[b], pos_s[b + 1])
            parts.append(jnp.where(t_id <= lim, s, NEG_FILL))
        sc = jnp.concatenate(parts, axis=0)
        m = jnp.max(sc, axis=-1, keepdims=True)
        e = jnp.where(sc > 0.5 * NEG_FILL, jnp.exp(sc - m), 0.0)
        l = jnp.sum(e, axis=-1, keepdims=True)
        some = l > 0.0
        inv = jnp.where(some, 1.0 / jnp.where(some, l, 1.0), 0.0)
        p_s[...] = e.astype(BF16)
        for g in range(groups):
            vm = vbuf[slot, 2 * g:2 * g + 2].reshape(width, hd)
            o = jnp.dot(p_s[g * ng:(g + 1) * ng, :], vm, preferred_element_type=F32)
            o_ref[pl.ds(pl.multiple_of((j * groups + g) * ng, ng), ng), :] = o * inv[g * ng:(g + 1) * ng, :]
        lse = jnp.where(some, m + jnp.log(jnp.where(some, l, 1.0)), NEG_FILL)
        lse_t = jnp.broadcast_to(lse, (groups * ng, 128)).T
        lse_ref[pl.ds(j, 1), :] = lse_t[0:1, :]
        k_o(j, slot).start()
        v_o(j, slot).start()

    for i in range(nbuf):
        j = nblk - nbuf + i
        k_o(j, j % nbuf).wait()
        v_o(j, j % nbuf).wait()


MESH_ID = pl.DeviceIdType.MESH


def merge_weights(a, b):
    top = jnp.maximum(a, b)
    ea, eb = jnp.exp(a - top), jnp.exp(b - top)
    tot = ea + eb
    return ea / tot, eb / tot, top + jnp.log(tot)


def columns(row):
    return jnp.broadcast_to(row, (128, 128)).T


def finish_kernel(cfg, o_hbm, lse_hbm, x_hbm, gain, wo_hbm, out_ref,
                  o_ref, lse_ref, x_ref, wo_v, r1, r1l, k2, k2l, s2, s2l, r2, r2l, wt, tmp, su, ku, ru, gat,
                  l_sem, s_d1, r_d1, s_dl, r_dl, s_x, r_x, s_xl, r_xl, s_y, r_y, s_ax, r_ax, s_ay, r_ay, s_f, r_f, s_d2, r_d2):
    nc, nq, hd = cfg
    dp, tp, sp = lax.axis_index('dp'), lax.axis_index('tp'), lax.axis_index('sp')
    core, xx = lax.rem(sp, 2), sp // 2
    partner = (dp, tp, xx * 2 + 1 - core)
    x_nbr = (dp, tp, (1 - xx) * 2 + core)
    y_nbr = (dp, 1 - tp, sp)

    def rcopy(src, dst, ss, rs, dev):
        return pltpu.make_async_remote_copy(src_ref=src, dst_ref=dst, send_sem=ss, recv_sem=rs, device_id=dev, device_id_type=MESH_ID)

    lse_load = pltpu.make_async_copy(lse_hbm, lse_ref, l_sem.at[0])
    o_load = pltpu.make_async_copy(o_hbm, o_ref, l_sem.at[1])
    wo_load = pltpu.make_async_copy(wo_hbm, wo_v, l_sem.at[2])
    x_load = pltpu.make_async_copy(x_hbm, x_ref, l_sem.at[3])
    for c in (lse_load, o_load, wo_load, x_load):
        c.start()
    barrier = pltpu.get_barrier_semaphore()
    for dev in (partner, x_nbr, y_nbr):
        pl.semaphore_signal(barrier, inc=1, device_id=dev, device_id_type=MESH_ID)
    pl.semaphore_wait(barrier, 3)

    def d1(c):
        other = 2 * c + 1 - core
        return rcopy(o_hbm.at[pl.ds(other * 128, 128)], r1.at[c], s_d1.at[c], r_d1.at[c], partner)

    dl = rcopy(lse_hbm, r1l, s_dl, r_dl, partner)

    def xs(c):
        return rcopy(s2.at[c], r2.at[c], s_x.at[c], r_x.at[c], x_nbr)

    def xl(c):
        return rcopy(s2l.at[c], r2l.at[c], s_xl.at[c], r_xl.at[c], x_nbr)

    def ys(c):
        return rcopy(su.at[c], ru.at[c], s_y.at[c], r_y.at[c], y_nbr)

    def blk(c, x, y):
        return c * 8 + core * 4 + x * 2 + y

    def ag(c, sems, rsems, dev):
        g = gat.at[blk(c, xx, tp)]
        return rcopy(g, g, sems.at[c], rsems.at[c], dev)

    def fw_y(c):
        g = gat.at[blk(c, 1 - xx, tp)]
        return rcopy(g, g, s_f.at[c], r_f.at[c], y_nbr)

    def fw_x(c):
        g = gat.at[blk(c, xx, 1 - tp)]
        return rcopy(g, g, s_f.at[c], r_f.at[c], x_nbr)

    def d2(c):
        g = gat.at[pl.ds(c * 8 + core * 4, 4)]
        return rcopy(g, g, s_d2.at[c], r_d2.at[c], partner)

    dl.start()

    @pl.loop(0, nc)
    def _(c):
        d1(c).start()

    for c in (lse_load, o_load, wo_load, x_load):
        c.wait()
    dl.wait_recv()

    def stage_a(c):
        d1(c).wait_recv()
        mine = 2 * c + core
        wa, wb, lse = merge_weights(lse_ref[pl.ds(mine, 1), :], r1l[pl.ds(mine, 1), :])
        wa, wb = columns(wa), columns(wb)
        r = pl.ds(pl.multiple_of(mine * 128, 128), 128)
        for i in range(hd // 128):
            col = slice(i * 128, (i + 1) * 128)
            tmp[i] = o_ref[r, col] * wa + r1[c, :, col] * wb
            k2[c, i] = tmp[i, pl.ds(pl.multiple_of(xx * 64, 64), 64), :]
            s2[c, i] = tmp[i, pl.ds(pl.multiple_of((1 - xx) * 64, 64), 64), :]
        k2l[c] = lse
        s2l[c] = lse
        xs(c).start()
        xl(c).start()

    def stage_b(c):
        xs(c).wait_recv()
        xl(c).wait_recv()
        wa, wb, _ = merge_weights(k2l[c], r2l[c])
        wt[0] = columns(wa)
        wt[1] = columns(wb)
        r = pl.ds(pl.multiple_of(xx * 64, 64), 64)
        wa, wb = wt[0, r, :], wt[1, r, :]
        for i in range(hd // 128):
            tmp[i, 0:64, :] = k2[c, i] * wa + r2[c, i] * wb
        parts = [tmp[i, pl.ds(h, 16, stride=nq), :] for h in range(nq) for i in range(hd // 128)]
        attn = jnp.concatenate(parts, axis=-1).astype(BF16)
        d_model = wo_v.shape[1]
        for n in range(d_model // 256):
            col = slice(n * 256, (n + 1) * 256)
            u = jnp.dot(attn, wo_v[:, col], preferred_element_type=F32)
            ku[c, :, col] = jnp.where(tp == 0, u[:8], u[8:])
            su[c, :, col] = jnp.where(tp == 0, u[8:], u[:8])
        ys(c).start()

    def stage_c(c):
        ys(c).wait_recv()
        u = ku[c] + ru[c]
        x = x_ref[pl.ds(pl.multiple_of(c * 64 + core * 32 + xx * 16, 16), 16), :].astype(F32)
        x = jnp.where(tp == 0, x[:8], x[8:])
        gat[blk(c, xx, tp)] = x + rms_scale(u, gain[...])
        ag(c, s_ax, r_ax, x_nbr).start()
        ag(c, s_ay, r_ay, y_nbr).start()

    def stage_d(c):
        ag(c, s_ax, r_ax, x_nbr).wait_recv()
        ag(c, s_ay, r_ay, y_nbr).wait_recv()

        @pl.when(lax.rem(c, 2) == 0)
        def _():
            fw_x(c).start()

        @pl.when(lax.rem(c, 2) == 1)
        def _():
            fw_y(c).start()

    def stage_e(c):
        @pl.when(lax.rem(c, 2) == 0)
        def _():
            fw_x(c).wait_recv()

        @pl.when(lax.rem(c, 2) == 1)
        def _():
            fw_y(c).wait_recv()

        d2(c).start()

    def stage_f(c):
        d2(c).wait_recv()
        for i in range(4):
            both = gat[pl.ds(c * 8 + 2 * i, 2)]
            out_ref[pl.ds(pl.multiple_of(c * 64 + 16 * i, 16), 16), :] = both.reshape(16, both.shape[-1]).astype(BF16)

    def at(t, lag, stage):
        c = t - lag

        @pl.when(jnp.logical_and(c >= 0, c < nc))
        def _():
            stage(c)

    @pl.loop(0, nc + 5)
    def _(t):
        at(t, 0, stage_a)
        at(t, 2, stage_c)
        at(t, 3, stage_d)
        at(t, 1, stage_b)
        at(t, 4, stage_e)
        at(t, 5, stage_f)

    dl.wait_send()

    @pl.loop(0, nc)
    def _(c):
        d1(c).wait_send()
        xs(c).wait_send()
        xl(c).wait_send()
        ys(c).wait_send()
        ag(c, s_ax, r_ax, x_nbr).wait_send()
        ag(c, s_ay, r_ay, y_nbr).wait_send()
        fw_x(c).wait_send()
        d2(c).wait_send()


def solution(mesh):
    cache_spec = P('dp', 'sp', 'tp', None)

    def local_step(x_in, cur_pos, w_pre, w_q, w_k, w_v, w_o, w_post, k_cache, v_cache):
        rows, seq, kv, hd = k_cache.shape
        d_model = x_in.shape[1]
        nq = w_q.shape[1] // hd
        half = hd // 2
        blk, nbuf, lag = 32, 8, 3
        nblk = rows // blk
        inv_freq = ROPE_BASE ** (-2.0 * jnp.arange(half, dtype=F32) / hd)
        ang = cur_pos.astype(F32)[:, None] * inv_freq[None, :]
        cos_t, sin_t = jnp.cos(ang), jnp.sin(ang)
        vmem, hbm = pl.BlockSpec(memory_space=pltpu.VMEM), pl.BlockSpec(memory_space=pl.ANY)
        dma = pltpu.SemaphoreType.DMA
        cfg = (rows, seq, kv, hd, blk, nbuf, lag)
        k_out, v_out, o_part, lse = pl.pallas_call(
            functools.partial(stream_kernel, cfg),
            name='stream',
            out_shape=[jax.ShapeDtypeStruct(k_cache.shape, BF16), jax.ShapeDtypeStruct(v_cache.shape, BF16),
                       jax.ShapeDtypeStruct((rows * nq, hd), F32), jax.ShapeDtypeStruct((nblk, blk * nq), F32)],
            in_specs=[pl.BlockSpec(memory_space=pltpu.SMEM), hbm, vmem, vmem, vmem, hbm, hbm, hbm, hbm, hbm],
            out_specs=[hbm, hbm, vmem, vmem],
            scratch_shapes=[
                pltpu.VMEM((rows, d_model), BF16), pltpu.VMEM((rows, d_model), BF16),
                pltpu.VMEM(w_q.shape, BF16), pltpu.VMEM(w_k.shape, BF16), pltpu.VMEM(w_v.shape, BF16),
                pltpu.VMEM((2, rows * nq, half), F32), pltpu.VMEM((2, rows * kv, half), F32), pltpu.VMEM((2, rows * kv, half), F32),
                pltpu.VMEM((nbuf, blk, seq, kv, hd), BF16), pltpu.VMEM((nbuf, blk, seq, kv, hd), BF16),
                pltpu.VMEM((blk * nq, 2 * seq * kv), BF16),
                dma((4,)), dma((nbuf,)), dma((nbuf,)), dma((nbuf,)), dma((nbuf,))],
            compiler_params=pltpu.CompilerParams(vmem_limit_bytes=66_000_000),
            cost_estimate=pl.CostEstimate(flops=10 ** 10, bytes_accessed=150_000_000, transcendentals=0),
        )(cur_pos, x_in, w_pre[None, :], cos_t, sin_t, w_q, w_k, w_v, k_cache, v_cache)

        nc, d_f32 = 8, (8, d_model)
        x_out = pl.pallas_call(
            functools.partial(finish_kernel, (nc, nq, hd)),
            name='finish',
            out_shape=jax.ShapeDtypeStruct(x_in.shape, BF16),
            in_specs=[hbm, hbm, hbm, vmem, hbm],
            out_specs=vmem,
            scratch_shapes=[
                pltpu.VMEM(o_part.shape, F32), pltpu.VMEM(lse.shape, F32), pltpu.VMEM(x_in.shape, BF16),
                pltpu.VMEM(w_o.shape, BF16), pltpu.VMEM((nc, 128, hd), F32), pltpu.VMEM(lse.shape, F32),
                pltpu.VMEM((nc, hd // 128, 64, 128), F32), pltpu.VMEM((nc, 1, 128), F32),
                pltpu.VMEM((nc, hd // 128, 64, 128), F32), pltpu.VMEM((nc, 1, 128), F32),
                pltpu.VMEM((nc, hd // 128, 64, 128), F32), pltpu.VMEM((nc, 1, 128), F32),
                pltpu.VMEM((2, 128, 128), F32), pltpu.VMEM((hd // 128, 128, 128), F32),
                pltpu.VMEM((nc,) + d_f32, F32), pltpu.VMEM((nc,) + d_f32, F32), pltpu.VMEM((nc,) + d_f32, F32),
                pltpu.VMEM((8 * nc,) + d_f32, F32),
                dma((4,)), dma((nc,)), dma((nc,)), dma, dma] + [dma((nc,))] * 14,
            compiler_params=pltpu.CompilerParams(vmem_limit_bytes=66_000_000, collective_id=0, has_side_effects=True),
        )(o_part, lse, x_in, w_post[None, :], w_o)
        return x_out, k_out, v_out

    return jax.shard_map(local_step, mesh=mesh,
                         in_specs=(P('dp', None), P('dp'), P(None), P(None, 'tp'), P(None, 'tp'), P(None, 'tp'), P('tp', None), P(None), cache_spec, cache_spec),
                         out_specs=(P('dp', None), cache_spec, cache_spec), check_vma=False)
```

```python
import functools

import jax
import jax.numpy as jnp
import numpy as np
from jax import lax
from jax.experimental import pallas as pl
from jax.experimental.pallas import tpu as pltpu
from jax.sharding import PartitionSpec as P

SOFT_CAP = 50.0
ROPE_BASE = 10000.0
NORM_EPS = 1e-6
NEG_FILL = -1e30
F32 = jnp.float32
BF16 = jnp.bfloat16


def rms_scale(tensor, gain_w):
    mean_sq = jnp.mean(tensor * tensor, axis=-1, keepdims=True)
    return tensor * lax.rsqrt(mean_sq + NORM_EPS) * (1.0 + gain_w)


def stream_kernel(cfg, pos_s, pos_v, freq, x_hbm, gain, wq_hbm, wk_hbm, wv_hbm, kc, vc, k_out, v_out, o_ref, lse_ref,
                  a_v, wq_v, wk_v, wv_v, cs, q_s, kn_s, vn_s, kbuf, vbuf, p_s,
                  w_sem, kin, vin, kout, vout):
    rows, seq, kv, hd, blk, nbuf, lag = cfg
    nblk = rows // blk
    groups = blk // 2
    half = hd // 2
    base = lax.axis_index('sp') * seq

    def k_in(j, s):
        return pltpu.make_async_copy(kc.at[pl.ds(j * blk, blk)], kbuf.at[s], kin.at[s])

    def v_in(j, s):
        return pltpu.make_async_copy(vc.at[pl.ds(j * blk, blk)], vbuf.at[s], vin.at[s])

    def k_o(j, s):
        return pltpu.make_async_copy(kbuf.at[s], k_out.at[pl.ds(j * blk, blk)], kout.at[s])

    def v_o(j, s):
        return pltpu.make_async_copy(vbuf.at[s], v_out.at[pl.ds(j * blk, blk)], vout.at[s])

    loads = [pltpu.make_async_copy(x_hbm, a_v, w_sem.at[0]), pltpu.make_async_copy(wq_hbm, wq_v, w_sem.at[1]),
             pltpu.make_async_copy(wk_hbm, wk_v, w_sem.at[2]), pltpu.make_async_copy(wv_hbm, wv_v, w_sem.at[3])]
    for c in loads:
        c.start()

    for i in range(rows // 128):
        ang = jnp.broadcast_to(pos_v[i:i + 1, :].astype(F32), (128, 128)).T * freq[...]
        cs[0, i * 128:(i + 1) * 128, :] = jnp.cos(ang)
        cs[1, i * 128:(i + 1) * 128, :] = jnp.sin(ang)

    loads[0].wait()
    step = 32

    @pl.loop(0, rows // step)
    def _(i):
        r = pl.ds(pl.multiple_of(i * step, step), step)
        a_v[r, :] = rms_scale(a_v[r, :].astype(F32), gain[...]).astype(BF16)

    for s in range(nbuf):
        k_in(s, s).start()
        v_in(s, s).start()

    nq = wq_v.shape[1] // hd

    def rope_store(acc, dst, h, stride):
        lo, hi = acc[:, :half], acc[:, half:]
        c, s = cs[0], cs[1]
        r_lo = (lo * c - hi * s).astype(BF16).astype(F32)
        r_hi = (hi * c + lo * s).astype(BF16).astype(F32)
        idx = pl.ds(h, rows, stride=stride)
        dst[0, idx, :] = r_lo
        dst[1, idx, :] = r_hi

    loads[1].wait()
    for h in range(nq):
        acc = jnp.dot(a_v[...], wq_v[:, h * hd:(h + 1) * hd], preferred_element_type=F32)
        rope_store(acc, q_s, h, nq)
    loads[2].wait()
    for h in range(kv):
        acc = jnp.dot(a_v[...], wk_v[:, h * hd:(h + 1) * hd], preferred_element_type=F32)
        rope_store(acc, kn_s, h, kv)
    loads[3].wait()
    for h in range(kv):
        acc = jnp.dot(a_v[...], wv_v[:, h * hd:(h + 1) * hd], preferred_element_type=F32)
        acc = acc.astype(BF16).astype(F32)
        idx = pl.ds(h, rows, stride=kv)
        vn_s[0, idx, :] = acc[:, :half]
        vn_s[1, idx, :] = acc[:, half:]

    ng = nq * 2
    width = 2 * seq * kv
    ri = lax.broadcasted_iota(jnp.int32, (ng, width), 0)
    ci = lax.broadcasted_iota(jnp.int32, (ng, width), 1)
    first = ri < nq
    same = jnp.logical_and(ri // nq == ci // (seq * kv), (ri % nq) // (nq // kv) == ci % kv)
    t_id = jnp.where(same, (ci % (seq * kv)) // kv + base, 1 << 20)
    scale = hd ** -0.5 / SOFT_CAP

    @pl.loop(0, nblk)
    def _(j):
        slot = lax.rem(j, nbuf)

        @pl.when(jnp.logical_and(j >= lag, j + nbuf - lag < nblk))
        def _():
            s2 = lax.rem(j - lag, nbuf)
            k_o(j - lag, s2).wait()
            k_in(j - lag + nbuf, s2).start()
            v_o(j - lag, s2).wait()
            v_in(j - lag + nbuf, s2).start()

        k_in(j, slot).wait()
        v_in(j, slot).wait()
        for i in range(blk):
            b = j * blk + i
            t = pos_s[b] - base
            hit = jnp.logical_and(t >= 0, t < seq)
            tt = jnp.clip(t, 0, seq - 1)
            r = pl.ds(kv * b, kv)
            row = jnp.concatenate([kn_s[0, r, :], kn_s[1, r, :]], axis=-1)
            kbuf[slot, i, tt] = jnp.where(hit, row, kbuf[slot, i, tt].astype(F32)).astype(BF16)
            row = jnp.concatenate([vn_s[0, r, :], vn_s[1, r, :]], axis=-1)
            vbuf[slot, i, tt] = jnp.where(hit, row, vbuf[slot, i, tt].astype(F32)).astype(BF16)

        parts = []
        for g in range(groups):
            r = pl.ds(pl.multiple_of((j * groups + g) * ng, ng), ng)
            qg = jnp.concatenate([q_s[0, r, :], q_s[1, r, :]], axis=-1).astype(BF16)
            km = kbuf[slot, 2 * g:2 * g + 2].reshape(width, hd)
            s = lax.dot_general(qg, km, (((1,), (1,)), ((), ())), preferred_element_type=F32)
            s = SOFT_CAP * jnp.tanh(s * scale)
            b = j * blk + 2 * g
            lim = jnp.where(first, pos_s[b], pos_s[b + 1])
            parts.append(jnp.where(t_id <= lim, s, NEG_FILL))
        sc = jnp.concatenate(parts, axis=0)
        m = jnp.max(sc, axis=-1, keepdims=True)
        e = jnp.where(sc > 0.5 * NEG_FILL, jnp.exp(sc - m), 0.0)
        l = jnp.sum(e, axis=-1, keepdims=True)
        some = l > 0.0
        inv = jnp.where(some, 1.0 / jnp.where(some, l, 1.0), 0.0)
        p_s[...] = e.astype(BF16)
        for g in range(groups):
            vm = vbuf[slot, 2 * g:2 * g + 2].reshape(width, hd)
            o = jnp.dot(p_s[g * ng:(g + 1) * ng, :], vm, preferred_element_type=F32)
            o_ref[pl.ds(pl.multiple_of((j * groups + g) * ng, ng), ng), :] = o * inv[g * ng:(g + 1) * ng, :]
        lse = jnp.where(some, m + jnp.log(jnp.where(some, l, 1.0)), NEG_FILL)
        lse_t = jnp.broadcast_to(lse, (groups * ng, 128)).T
        lse_ref[pl.ds(j, 1), :] = lse_t[0:1, :]
        k_o(j, slot).start()
        v_o(j, slot).start()

    for i in range(nbuf):
        j = nblk - nbuf + i
        k_o(j, j % nbuf).wait()
        v_o(j, j % nbuf).wait()


MESH_ID = pl.DeviceIdType.MESH


def merge_weights(a, b):
    top = jnp.maximum(a, b)
    ea, eb = jnp.exp(a - top), jnp.exp(b - top)
    tot = ea + eb
    return ea / tot, eb / tot, top + jnp.log(tot)


def columns(row):
    return jnp.broadcast_to(row, (128, 128)).T


def finish_kernel(cfg, o_ref, lse_ref, x_hbm, gain, wo_hbm, out_ref,
                  x_ref, wo_v, r1, r1l, k2, k2l, s2, s2l, r2, r2l, wt, tmp, su, ku, ru, gat,
                  l_sem, s_d1, r_d1, s_dl, r_dl, s_x, r_x, s_xl, r_xl, s_y, r_y, s_ax, r_ax, s_ay, r_ay, s_f, r_f, s_d2, r_d2):
    nc, nq, hd = cfg
    dp, tp, sp = lax.axis_index('dp'), lax.axis_index('tp'), lax.axis_index('sp')
    core, xx = lax.rem(sp, 2), sp // 2
    partner = (dp, tp, xx * 2 + 1 - core)
    x_nbr = (dp, tp, (1 - xx) * 2 + core)
    y_nbr = (dp, 1 - tp, sp)

    def rcopy(src, dst, ss, rs, dev):
        return pltpu.make_async_remote_copy(src_ref=src, dst_ref=dst, send_sem=ss, recv_sem=rs, device_id=dev, device_id_type=MESH_ID)

    wo_load = pltpu.make_async_copy(wo_hbm, wo_v, l_sem.at[0])
    x_load = pltpu.make_async_copy(x_hbm, x_ref, l_sem.at[1])
    wo_load.start()
    x_load.start()
    barrier = pltpu.get_barrier_semaphore()
    for dev in (partner, x_nbr, y_nbr):
        pl.semaphore_signal(barrier, inc=1, device_id=dev, device_id_type=MESH_ID)
    pl.semaphore_wait(barrier, 3)

    def d1(c):
        other = 2 * c + 1 - core
        return rcopy(o_ref.at[pl.ds(other * 128, 128)], r1.at[c], s_d1.at[c], r_d1.at[c], partner)

    dl = rcopy(lse_ref, r1l, s_dl, r_dl, partner)

    def xs(c):
        return rcopy(s2.at[c], r2.at[c], s_x.at[c], r_x.at[c], x_nbr)

    def xl(c):
        return rcopy(s2l.at[c], r2l.at[c], s_xl.at[c], r_xl.at[c], x_nbr)

    def ys(c):
        return rcopy(su.at[c], ru.at[c], s_y.at[c], r_y.at[c], y_nbr)

    def blk(c, x, y):
        return c * 8 + core * 4 + x * 2 + y

    def ag(c, sems, rsems, dev):
        g = gat.at[blk(c, xx, tp)]
        return rcopy(g, g, sems.at[c], rsems.at[c], dev)

    def fw_y(c):
        g = gat.at[blk(c, 1 - xx, tp)]
        return rcopy(g, g, s_f.at[c], r_f.at[c], y_nbr)

    def fw_x(c):
        g = gat.at[blk(c, xx, 1 - tp)]
        return rcopy(g, g, s_f.at[c], r_f.at[c], x_nbr)

    def d2(c):
        g = gat.at[pl.ds(c * 8 + core * 4, 4)]
        return rcopy(g, g, s_d2.at[c], r_d2.at[c], partner)

    dl.start()

    @pl.loop(0, nc)
    def _(c):
        d1(c).start()

    dl.wait_recv()

    def stage_a(c):
        d1(c).wait_recv()
        mine = 2 * c + core
        wa, wb, lse = merge_weights(lse_ref[pl.ds(mine, 1), :], r1l[pl.ds(mine, 1), :])
        wa, wb = columns(wa), columns(wb)
        r = pl.ds(pl.multiple_of(mine * 128, 128), 128)
        for i in range(hd // 128):
            col = slice(i * 128, (i + 1) * 128)
            tmp[i] = o_ref[r, col] * wa + r1[c, :, col] * wb
            k2[c, i] = tmp[i, pl.ds(pl.multiple_of(xx * 64, 64), 64), :]
            s2[c, i] = tmp[i, pl.ds(pl.multiple_of((1 - xx) * 64, 64), 64), :]
        k2l[c] = lse
        s2l[c] = lse
        xs(c).start()
        xl(c).start()

    def stage_b(c):
        xs(c).wait_recv()
        xl(c).wait_recv()
        wa, wb, _ = merge_weights(k2l[c], r2l[c])
        wt[0] = columns(wa)
        wt[1] = columns(wb)
        r = pl.ds(pl.multiple_of(xx * 64, 64), 64)
        wa, wb = wt[0, r, :], wt[1, r, :]
        for i in range(hd // 128):
            tmp[i, 0:64, :] = k2[c, i] * wa + r2[c, i] * wb
        parts = [tmp[i, pl.ds(h, 16, stride=nq), :] for h in range(nq) for i in range(hd // 128)]
        attn = jnp.concatenate(parts, axis=-1).astype(BF16)
        d_model = wo_v.shape[1]
        for n in range(d_model // 256):
            col = slice(n * 256, (n + 1) * 256)
            u = jnp.dot(attn, wo_v[:, col], preferred_element_type=F32)
            ku[c, :, col] = jnp.where(tp == 0, u[:8], u[8:])
            su[c, :, col] = jnp.where(tp == 0, u[8:], u[:8])
        ys(c).start()

    def stage_c(c):
        ys(c).wait_recv()
        u = ku[c] + ru[c]
        x = x_ref[pl.ds(pl.multiple_of(c * 64 + core * 32 + xx * 16, 16), 16), :].astype(F32)
        x = jnp.where(tp == 0, x[:8], x[8:])
        gat[blk(c, xx, tp)] = x + rms_scale(u, gain[...])
        ag(c, s_ax, r_ax, x_nbr).start()
        ag(c, s_ay, r_ay, y_nbr).start()

    def stage_d(c):
        ag(c, s_ax, r_ax, x_nbr).wait_recv()
        ag(c, s_ay, r_ay, y_nbr).wait_recv()

        @pl.when(lax.rem(c, 3) != 2)
        def _():
            fw_x(c).start()

        @pl.when(lax.rem(c, 3) == 2)
        def _():
            fw_y(c).start()

    def stage_e(c):
        @pl.when(lax.rem(c, 3) != 2)
        def _():
            fw_x(c).wait_recv()

        @pl.when(lax.rem(c, 3) == 2)
        def _():
            fw_y(c).wait_recv()

        d2(c).start()

    def stage_f(c):
        d2(c).wait_recv()
        for i in range(4):
            both = gat[pl.ds(c * 8 + 2 * i, 2)]
            out_ref[pl.ds(pl.multiple_of(c * 64 + 16 * i, 16), 16), :] = both.reshape(16, both.shape[-1]).astype(BF16)

    def at(t, lag, stage):
        c = t - lag

        @pl.when(jnp.logical_and(c >= 0, c < nc))
        def _():
            stage(c)

    @pl.loop(0, nc + 9)
    def _(t):
        at(t, 0, stage_a)

        @pl.when(t == 2)
        def _():
            wo_load.wait()
            x_load.wait()

        at(t, 2, stage_b)
        at(t, 4, stage_c)
        at(t, 6, stage_d)
        at(t, 8, stage_e)
        at(t, 9, stage_f)

    dl.wait_send()

    @pl.loop(0, nc)
    def _(c):
        d1(c).wait_send()
        xs(c).wait_send()
        xl(c).wait_send()
        ys(c).wait_send()
        ag(c, s_ax, r_ax, x_nbr).wait_send()
        ag(c, s_ay, r_ay, y_nbr).wait_send()
        fw_x(c).wait_send()
        d2(c).wait_send()


def solution(mesh):
    cache_spec = P('dp', 'sp', 'tp', None)

    def local_step(x_in, cur_pos, w_pre, w_q, w_k, w_v, w_o, w_post, k_cache, v_cache):
        rows, seq, kv, hd = k_cache.shape
        d_model = x_in.shape[1]
        nq = w_q.shape[1] // hd
        half = hd // 2
        blk, nbuf, lag = 32, 8, 3
        nblk = rows // blk
        inv_freq = (ROPE_BASE ** (-2.0 * np.arange(half) / hd)).astype(np.float32)[None, :]
        vmem, hbm = pl.BlockSpec(memory_space=pltpu.VMEM), pl.BlockSpec(memory_space=pl.ANY)
        dma = pltpu.SemaphoreType.DMA
        cfg = (rows, seq, kv, hd, blk, nbuf, lag)
        k_out, v_out, o_part, lse = pl.pallas_call(
            functools.partial(stream_kernel, cfg),
            name='stream',
            out_shape=[jax.ShapeDtypeStruct(k_cache.shape, BF16), jax.ShapeDtypeStruct(v_cache.shape, BF16),
                       pltpu.VMEM((rows * nq, hd), F32), pltpu.VMEM((nblk, blk * nq), F32)],
            in_specs=[pl.BlockSpec(memory_space=pltpu.SMEM), vmem, vmem, hbm, vmem, hbm, hbm, hbm, hbm, hbm],
            out_specs=[hbm, hbm, vmem, vmem],
            scratch_shapes=[
                pltpu.VMEM((rows, d_model), BF16),
                pltpu.VMEM(w_q.shape, BF16), pltpu.VMEM(w_k.shape, BF16), pltpu.VMEM(w_v.shape, BF16),
                pltpu.VMEM((2, rows, half), F32),
                pltpu.VMEM((2, rows * nq, half), F32), pltpu.VMEM((2, rows * kv, half), F32), pltpu.VMEM((2, rows * kv, half), F32),
                pltpu.VMEM((nbuf, blk, seq, kv, hd), BF16), pltpu.VMEM((nbuf, blk, seq, kv, hd), BF16),
                pltpu.VMEM((blk * nq, 2 * seq * kv), BF16),
                dma((4,)), dma((nbuf,)), dma((nbuf,)), dma((nbuf,)), dma((nbuf,))],
            compiler_params=pltpu.CompilerParams(vmem_limit_bytes=57_000_000),
            cost_estimate=pl.CostEstimate(flops=10 ** 10, bytes_accessed=150_000_000, transcendentals=0),
        )(cur_pos, cur_pos.reshape(rows // 128, 128), inv_freq, x_in, w_pre, w_q, w_k, w_v, k_cache, v_cache)

        nc, d_f32 = 8, (8, d_model)
        x_out = pl.pallas_call(
            functools.partial(finish_kernel, (nc, nq, hd)),
            name='finish',
            out_shape=pltpu.VMEM(x_in.shape, BF16),
            in_specs=[vmem, vmem, hbm, vmem, hbm],
            out_specs=vmem,
            scratch_shapes=[
                pltpu.VMEM(x_in.shape, BF16),
                pltpu.VMEM(w_o.shape, BF16), pltpu.VMEM((nc, 128, hd), F32), pltpu.VMEM(lse.shape, F32),
                pltpu.VMEM((nc, hd // 128, 64, 128), F32), pltpu.VMEM((nc, 1, 128), F32),
                pltpu.VMEM((nc, hd // 128, 64, 128), F32), pltpu.VMEM((nc, 1, 128), F32),
                pltpu.VMEM((nc, hd // 128, 64, 128), F32), pltpu.VMEM((nc, 1, 128), F32),
                pltpu.VMEM((2, 128, 128), F32), pltpu.VMEM((hd // 128, 128, 128), F32),
                pltpu.VMEM((nc,) + d_f32, F32), pltpu.VMEM((nc,) + d_f32, F32), pltpu.VMEM((nc,) + d_f32, F32),
                pltpu.VMEM((8 * nc,) + d_f32, F32),
                dma((2,)), dma((nc,)), dma((nc,)), dma, dma] + [dma((nc,))] * 14,
            compiler_params=pltpu.CompilerParams(vmem_limit_bytes=50_000_000, collective_id=0, has_side_effects=True),
            cost_estimate=pl.CostEstimate(flops=10 ** 10, bytes_accessed=100_000_000, transcendentals=0),
        )(o_part, lse, x_in, w_post, w_o)
        return x_out, k_out, v_out

    return jax.shard_map(local_step, mesh=mesh,
                         in_specs=(P('dp', None), P('dp'), P(None), P(None, 'tp'), P(None, 'tp'), P(None, 'tp'), P('tp', None), P(None), cache_spec, cache_spec),
                         out_specs=(P('dp', None), cache_spec, cache_spec), check_vma=False)
```

```python
import functools

import jax
import jax.numpy as jnp
import numpy as np
from jax import lax
from jax.experimental import pallas as pl
from jax.experimental.pallas import tpu as pltpu
from jax.sharding import PartitionSpec as P

SOFT_CAP = 50.0
ROPE_BASE = 10000.0
NORM_EPS = 1e-6
NEG_FILL = -1e30
F32 = jnp.float32
BF16 = jnp.bfloat16


def rms_scale(tensor, gain_w):
    mean_sq = jnp.mean(tensor * tensor, axis=-1, keepdims=True)
    return tensor * lax.rsqrt(mean_sq + NORM_EPS) * (1.0 + gain_w)


def score_ids(nq, seq, kv, base):
    ng, width = nq * 2, 2 * seq * kv
    ri = lax.broadcasted_iota(jnp.int32, (ng, width), 0)
    ci = lax.broadcasted_iota(jnp.int32, (ng, width), 1)
    same = jnp.logical_and(ri // nq == ci // (seq * kv), (ri % nq) // (nq // kv) == ci % kv)
    return ng, width, ri < nq, jnp.where(same, (ci % (seq * kv)) // kv + base, 1 << 20)


def attend(k_of, v_of, q_of, lim_of, put, groups, ng, t_id, p_s, new=None):
    scale = k_of(0).shape[1] ** -0.5 / SOFT_CAP
    parts, hits = [], []
    if new is not None:
        q_lo, q_hi, k_lo, k_hi, v_lo, v_hi = new
        s_new = SOFT_CAP * jnp.tanh(jnp.sum(q_lo * k_lo + q_hi * k_hi, axis=-1, keepdims=True) * scale)
    for g in range(groups):
        s = lax.dot_general(q_of(g).astype(BF16), k_of(g), (((1,), (1,)), ((), ())), preferred_element_type=F32)
        s = SOFT_CAP * jnp.tanh(s * scale)
        lim = lim_of(g)
        if new is not None:
            hit = t_id == lim
            s = jnp.where(hit, s_new[g * ng:(g + 1) * ng, :], s)
            hits.append(jnp.where(hit, 1.0, 0.0))
        parts.append(jnp.where(t_id <= lim, s, NEG_FILL))
    sc = jnp.concatenate(parts, axis=0)
    m = jnp.max(sc, axis=-1, keepdims=True)
    e = jnp.where(sc > 0.5 * NEG_FILL, jnp.exp(sc - m), 0.0)
    l = jnp.sum(e, axis=-1, keepdims=True)
    some = l > 0.0
    inv = jnp.where(some, 1.0 / jnp.where(some, l, 1.0), 0.0)
    if new is not None:
        hit = jnp.concatenate(hits, axis=0)
        e_new = jnp.sum(e * hit, axis=-1, keepdims=True)
        e = e * (1.0 - hit)
        own = jnp.concatenate([v_lo * e_new, v_hi * e_new], axis=-1)
    p_s[...] = e.astype(BF16)
    for g in range(groups):
        r = slice(g * ng, (g + 1) * ng)
        o = jnp.dot(p_s[r, :], v_of(g), preferred_element_type=F32)
        if new is not None:
            o = o + own[r, :]
        put(g, o * inv[r, :])
    lse = jnp.where(some, m + jnp.log(jnp.where(some, l, 1.0)), NEG_FILL)
    return jnp.broadcast_to(lse, (groups * ng, 128)).T[0:1, :]


def stream_kernel(cfg, pos_s, pos_v, freq, x_hbm, gain, wq_hbm, wk_hbm, wv_hbm, kc, vc, k_out, v_out, o_ref, lse_ref, q_c, ke_c, ve_c,
                  a_v, wq_v, wk_v, wv_v, cs, q_s, kn_s, vn_s, kbuf, vbuf, p_s,
                  w_sem, kin, vin, kout, vout):
    rows, early, seq, kv, hd, blk, nbuf, lag = cfg
    late = rows - early
    nblk = early // blk
    groups = blk // 2
    half = hd // 2
    base = lax.axis_index('sp') * seq

    def k_in(j, s):
        return pltpu.make_async_copy(kc.at[pl.ds(j * blk, blk)], kbuf.at[s], kin.at[s])

    def v_in(j, s):
        return pltpu.make_async_copy(vc.at[pl.ds(j * blk, blk)], vbuf.at[s], vin.at[s])

    def k_o(j, s):
        return pltpu.make_async_copy(kbuf.at[s], k_out.at[pl.ds(j * blk, blk)], kout.at[s])

    def v_o(j, s):
        return pltpu.make_async_copy(vbuf.at[s], v_out.at[pl.ds(j * blk, blk)], vout.at[s])

    loads = [pltpu.make_async_copy(x_hbm, a_v, w_sem.at[0]), pltpu.make_async_copy(wq_hbm, wq_v, w_sem.at[1]),
             pltpu.make_async_copy(wk_hbm, wk_v, w_sem.at[2]), pltpu.make_async_copy(wv_hbm, wv_v, w_sem.at[3])]
    for c in loads:
        c.start()

    for i in range(rows // 128):
        ang = jnp.broadcast_to(pos_v[i:i + 1, :].astype(F32), (128, 128)).T * freq[...]
        cs[0, i * 128:(i + 1) * 128, :] = jnp.cos(ang)
        cs[1, i * 128:(i + 1) * 128, :] = jnp.sin(ang)

    loads[0].wait()
    step = 32

    @pl.loop(0, rows // step)
    def _(i):
        r = pl.ds(pl.multiple_of(i * step, step), step)
        a_v[r, :] = rms_scale(a_v[r, :].astype(F32), gain[...]).astype(BF16)

    for s in range(nbuf):
        k_in(s, s).start()
        v_in(s, s).start()

    nq = wq_v.shape[1] // hd

    def spread(pair, dst, h, stride, dst_c, heads):
        for i, part in enumerate(pair):
            part = part.astype(BF16).astype(F32)
            dst[i, pl.ds(h, early, stride=stride), :] = part[:early]
            for hc in heads:
                dst_c[i, pl.ds(hc, late, stride=nq), :] = part[early:]

    def rope(acc):
        lo, hi = acc[:, :half], acc[:, half:]
        return lo * cs[0] - hi * cs[1], hi * cs[0] + lo * cs[1]

    share = nq // kv
    loads[1].wait()
    for h in range(nq):
        acc = jnp.dot(a_v[...], wq_v[:, h * hd:(h + 1) * hd], preferred_element_type=F32)
        spread(rope(acc), q_s, h, nq, q_c, (h,))
    loads[2].wait()
    for h in range(kv):
        acc = jnp.dot(a_v[...], wk_v[:, h * hd:(h + 1) * hd], preferred_element_type=F32)
        spread(rope(acc), kn_s, h, kv, ke_c, range(h * share, (h + 1) * share))
    loads[3].wait()
    for h in range(kv):
        acc = jnp.dot(a_v[...], wv_v[:, h * hd:(h + 1) * hd], preferred_element_type=F32)
        spread((acc[:, :half], acc[:, half:]), vn_s, h, kv, ve_c, range(h * share, (h + 1) * share))

    ng, width, first, t_id = score_ids(nq, seq, kv, base)

    @pl.loop(0, nblk)
    def _(j):
        slot = lax.rem(j, nbuf)

        @pl.when(jnp.logical_and(j >= lag, j + nbuf - lag < nblk))
        def _():
            s2 = lax.rem(j - lag, nbuf)
            k_o(j - lag, s2).wait()
            k_in(j - lag + nbuf, s2).start()
            v_o(j - lag, s2).wait()
            v_in(j - lag + nbuf, s2).start()

        k_in(j, slot).wait()
        v_in(j, slot).wait()
        for i in range(blk):
            b = j * blk + i
            t = pos_s[b] - base
            hit = jnp.logical_and(t >= 0, t < seq)
            tt = jnp.clip(t, 0, seq - 1)
            r = pl.ds(kv * b, kv)
            row = jnp.concatenate([kn_s[0, r, :], kn_s[1, r, :]], axis=-1)
            kbuf[slot, i, tt] = jnp.where(hit, row, kbuf[slot, i, tt].astype(F32)).astype(BF16)
            row = jnp.concatenate([vn_s[0, r, :], vn_s[1, r, :]], axis=-1)
            vbuf[slot, i, tt] = jnp.where(hit, row, vbuf[slot, i, tt].astype(F32)).astype(BF16)

        def q_of(g):
            r = pl.ds(pl.multiple_of((j * groups + g) * ng, ng), ng)
            return jnp.concatenate([q_s[0, r, :], q_s[1, r, :]], axis=-1)

        def lim_of(g):
            return jnp.where(first, pos_s[j * blk + 2 * g], pos_s[j * blk + 2 * g + 1])

        def put(g, o):
            o_ref[pl.ds(pl.multiple_of((j * groups + g) * ng, ng), ng), :] = o

        lse_ref[j] = attend(lambda g: kbuf[slot, 2 * g:2 * g + 2].reshape(width, hd), lambda g: vbuf[slot, 2 * g:2 * g + 2].reshape(width, hd),
                            q_of, lim_of, put, groups, ng, t_id, p_s)
        k_o(j, slot).start()
        v_o(j, slot).start()

    for i in range(nbuf):
        j = nblk - nbuf + i
        k_o(j, j % nbuf).wait()
        v_o(j, j % nbuf).wait()


MESH_ID = pl.DeviceIdType.MESH


def merge_weights(a, b):
    top = jnp.maximum(a, b)
    ea, eb = jnp.exp(a - top), jnp.exp(b - top)
    tot = ea + eb
    return ea / tot, eb / tot, top + jnp.log(tot)


def columns(row):
    return jnp.broadcast_to(row, (128, 128)).T


def finish_kernel(cfg, pos_s, o_in, lse_in, q_c, ke_c, ve_c, x_hbm, gain, wo_hbm, kc, vc, out_ref, kv_buf,
                  o_ref, lse_ref, p_s, x_ref, wo_v, r1, r1l, k2, k2l, s2, s2l, r2, r2l, wt, tmp, su, ku, ru, gat,
                  l_sem, c_sem, s_d1, r_d1, s_dl, r_dl, s_x, r_x, s_xl, r_xl, s_y, r_y, s_ax, r_ax, s_ay, r_ay, s_f, r_f, s_d2, r_d2):
    nc, nq, hd, early, blk = cfg
    kbuf, vbuf = kv_buf.at[0], kv_buf.at[1]
    seq, kv = kc.shape[1], kc.shape[2]
    n_early, n_late = early // blk, kbuf.shape[0] // blk
    span = blk * nq
    dp, tp, sp = lax.axis_index('dp'), lax.axis_index('tp'), lax.axis_index('sp')
    core, xx = lax.rem(sp, 2), sp // 2
    partner = (dp, tp, xx * 2 + 1 - core)
    x_nbr = (dp, tp, (1 - xx) * 2 + core)
    y_nbr = (dp, 1 - tp, sp)

    def rcopy(src, dst, ss, rs, dev):
        return pltpu.make_async_remote_copy(src_ref=src, dst_ref=dst, send_sem=ss, recv_sem=rs, device_id=dev, device_id_type=MESH_ID)

    wo_load = pltpu.make_async_copy(wo_hbm, wo_v, l_sem.at[0])
    x_load = pltpu.make_async_copy(x_hbm, x_ref, l_sem.at[1])
    wo_load.start()
    x_load.start()

    def k_in(j):
        return pltpu.make_async_copy(kc.at[pl.ds(early + j * blk, blk)], kbuf.at[pl.ds(j * blk, blk)], c_sem.at[0, j])

    def v_in(j):
        return pltpu.make_async_copy(vc.at[pl.ds(early + j * blk, blk)], vbuf.at[pl.ds(j * blk, blk)], c_sem.at[1, j])

    @pl.loop(0, n_late)
    def _(j):
        k_in(j).start()
        v_in(j).start()

    @pl.loop(0, n_early)
    def _(j):
        r = pl.ds(pl.multiple_of(j * span, span), span)
        o_ref[r, :] = o_in[r, :]
        lse_ref[j] = lse_in[j]

    barrier = pltpu.get_barrier_semaphore()
    for dev in (partner, x_nbr, y_nbr):
        pl.semaphore_signal(barrier, inc=1, device_id=dev, device_id_type=MESH_ID)
    pl.semaphore_wait(barrier, 3)

    def d1(c):
        other = 2 * c + 1 - core
        return rcopy(o_ref.at[pl.ds(other * 128, 128)], r1.at[c], s_d1.at[c], r_d1.at[c], partner)

    def dl(c):
        other = 2 * c + 1 - core
        return rcopy(lse_ref.at[other], r1l.at[other], s_dl.at[c], r_dl.at[c], partner)

    def xs(c):
        return rcopy(s2.at[c], r2.at[c], s_x.at[c], r_x.at[c], x_nbr)

    def xl(c):
        return rcopy(s2l.at[c], r2l.at[c], s_xl.at[c], r_xl.at[c], x_nbr)

    def ys(c):
        return rcopy(su.at[c], ru.at[c], s_y.at[c], r_y.at[c], y_nbr)

    def slab(c, x, y):
        return c * 8 + core * 4 + x * 2 + y

    def ag(c, sems, rsems, dev):
        g = gat.at[slab(c, xx, tp)]
        return rcopy(g, g, sems.at[c], rsems.at[c], dev)

    def fw_y(c):
        g = gat.at[slab(c, 1 - xx, tp)]
        return rcopy(g, g, s_f.at[c], r_f.at[c], y_nbr)

    def fw_x(c):
        g = gat.at[slab(c, xx, 1 - tp)]
        return rcopy(g, g, s_f.at[c], r_f.at[c], x_nbr)

    def d2(c):
        g = gat.at[pl.ds(c * 8 + core * 4, 4)]
        return rcopy(g, g, s_d2.at[c], r_d2.at[c], partner)

    @pl.loop(0, n_early // 2)
    def _(c):
        dl(c).start()
        d1(c).start()

    ng, width, first, t_id = score_ids(nq, seq, kv, sp * seq)
    groups = blk // 2

    def stage_attend(j):
        k_in(j).wait()
        v_in(j).wait()
        rows = pl.ds(pl.multiple_of(j * span, span), span)
        at0 = pl.multiple_of(early * nq + j * span, span)
        new = (q_c[0, rows, :], q_c[1, rows, :], ke_c[0, rows, :], ke_c[1, rows, :], ve_c[0, rows, :], ve_c[1, rows, :])

        def q_of(g):
            r = pl.ds(pl.multiple_of(j * span + g * ng, ng), ng)
            return jnp.concatenate([q_c[0, r, :], q_c[1, r, :]], axis=-1)

        def lim_of(g):
            b = early + j * blk + 2 * g
            return jnp.where(first, pos_s[b], pos_s[b + 1])

        def put(g, o):
            o_ref[pl.ds(pl.multiple_of(at0 + g * ng, ng), ng), :] = o

        lse_ref[n_early + j] = attend(lambda g: kbuf[pl.ds(j * blk + 2 * g, 2)].reshape(width, hd),
                                      lambda g: vbuf[pl.ds(j * blk + 2 * g, 2)].reshape(width, hd),
                                      q_of, lim_of, put, groups, ng, t_id, p_s, new)

        @pl.when(lax.rem(j, 2) == 1)
        def _():
            c = (n_early + j) // 2
            dl(c).start()
            d1(c).start()

    def stage_a(c):
        d1(c).wait_recv()
        dl(c).wait_recv()
        mine = 2 * c + core
        wa, wb, lse = merge_weights(lse_ref[mine], r1l[mine])
        wa, wb = columns(wa), columns(wb)
        r = pl.ds(pl.multiple_of(mine * 128, 128), 128)
        for i in range(hd // 128):
            col = slice(i * 128, (i + 1) * 128)
            tmp[i] = o_ref[r, col] * wa + r1[c, :, col] * wb
            k2[c, i] = tmp[i, pl.ds(pl.multiple_of(xx * 64, 64), 64), :]
            s2[c, i] = tmp[i, pl.ds(pl.multiple_of((1 - xx) * 64, 64), 64), :]
        k2l[c] = lse
        s2l[c] = lse
        xs(c).start()
        xl(c).start()

    def stage_b(c):
        xs(c).wait_recv()
        xl(c).wait_recv()
        wa, wb, _ = merge_weights(k2l[c], r2l[c])
        wt[0] = columns(wa)
        wt[1] = columns(wb)
        r = pl.ds(pl.multiple_of(xx * 64, 64), 64)
        wa, wb = wt[0, r, :], wt[1, r, :]
        for i in range(hd // 128):
            tmp[i, 0:64, :] = k2[c, i] * wa + r2[c, i] * wb
        parts = [tmp[i, pl.ds(h, 16, stride=nq), :] for h in range(nq) for i in range(hd // 128)]
        attn = jnp.concatenate(parts, axis=-1).astype(BF16)
        d_model = wo_v.shape[1]
        for n in range(d_model // 256):
            col = slice(n * 256, (n + 1) * 256)
            u = jnp.dot(attn, wo_v[:, col], preferred_element_type=F32)
            ku[c, :, col] = jnp.where(tp == 0, u[:8], u[8:])
            su[c, :, col] = jnp.where(tp == 0, u[8:], u[:8])
        ys(c).start()

    def stage_c(c):
        ys(c).wait_recv()
        u = ku[c] + ru[c]
        x = x_ref[pl.ds(pl.multiple_of(c * 64 + core * 32 + xx * 16, 16), 16), :].astype(F32)
        x = jnp.where(tp == 0, x[:8], x[8:])
        gat[slab(c, xx, tp)] = x + rms_scale(u, gain[...])
        ag(c, s_ax, r_ax, x_nbr).start()
        ag(c, s_ay, r_ay, y_nbr).start()

    def stage_d(c):
        ag(c, s_ax, r_ax, x_nbr).wait_recv()
        ag(c, s_ay, r_ay, y_nbr).wait_recv()

        @pl.when(lax.rem(c, 3) != 2)
        def _():
            fw_x(c).start()

        @pl.when(lax.rem(c, 3) == 2)
        def _():
            fw_y(c).start()

    def stage_e(c):
        @pl.when(lax.rem(c, 3) != 2)
        def _():
            fw_x(c).wait_recv()

        @pl.when(lax.rem(c, 3) == 2)
        def _():
            fw_y(c).wait_recv()

        d2(c).start()

    def stage_f(c):
        d2(c).wait_recv()
        for i in range(4):
            both = gat[pl.ds(c * 8 + 2 * i, 2)]
            out_ref[pl.ds(pl.multiple_of(c * 64 + 16 * i, 16), 16), :] = both.reshape(16, both.shape[-1]).astype(BF16)

    def at(t, lag, stage):
        c = t - lag

        @pl.when(jnp.logical_and(c >= 0, c < nc))
        def _():
            stage(c)

    @pl.loop(0, nc + 9)
    def _(t):
        at(t, 0, stage_a)

        @pl.when(t == 2)
        def _():
            wo_load.wait()
            x_load.wait()

        at(t, 2, stage_b)
        at(t, 4, stage_c)
        at(t, 6, stage_d)
        at(t, 8, stage_e)
        at(t, 9, stage_f)

        @pl.when(t < n_late)
        def _():
            stage_attend(t)

    @pl.loop(0, nc)
    def _(c):
        d1(c).wait_send()
        dl(c).wait_send()
        xs(c).wait_send()
        xl(c).wait_send()
        ys(c).wait_send()
        ag(c, s_ax, r_ax, x_nbr).wait_send()
        ag(c, s_ay, r_ay, y_nbr).wait_send()
        fw_x(c).wait_send()
        d2(c).wait_send()


def close_kernel(cfg, pos_s, x_ref, ke_c, ve_c, kv_in, k_part, v_part, x_out, k_out, v_out, kv_buf, x_sem, o_sem):
    kb, vb = kv_buf.at[0], kv_buf.at[1]
    early, blk, seq, nq, kv = cfg
    base = lax.axis_index('sp') * seq
    n_late = kb.shape[0] // blk
    copy = pltpu.make_async_copy(x_ref, x_out, x_sem)
    copy.start()

    def out(i, buf, dst, j):
        return pltpu.make_async_copy(buf.at[pl.ds(j * blk, blk)], dst.at[pl.ds(early + j * blk, blk)], o_sem.at[i, j])

    @pl.loop(0, n_late)
    def _(j):
        for i in range(blk):
            b = j * blk + i
            t = pos_s[early + b] - base
            hit = jnp.logical_and(t >= 0, t < seq)
            tt = jnp.clip(t, 0, seq - 1)
            r = pl.ds(nq * b, kv, stride=nq // kv)
            for buf, new in ((kb, ke_c), (vb, ve_c)):
                row = jnp.concatenate([new[0, r, :], new[1, r, :]], axis=-1)
                buf[b, tt] = jnp.where(hit, row, buf[b, tt].astype(F32)).astype(BF16)
        out(0, kb, k_out, j).start()
        out(1, vb, v_out, j).start()

    @pl.loop(0, n_late)
    def _(j):
        out(0, kb, k_out, j).wait()
        out(1, vb, v_out, j).wait()

    copy.wait()


def solution(mesh):
    cache_spec = P('dp', 'sp', 'tp', None)

    def local_step(x_in, cur_pos, w_pre, w_q, w_k, w_v, w_o, w_post, k_cache, v_cache):
        rows, seq, kv, hd = k_cache.shape
        d_model = x_in.shape[1]
        nq = w_q.shape[1] // hd
        half = hd // 2
        blk, nbuf, lag = 32, 8, 3
        late = 192
        early = rows - late
        nblk = early // blk
        new_shape = pltpu.VMEM((2, late * nq, half), F32)
        inv_freq = (ROPE_BASE ** (-2.0 * np.arange(half) / hd)).astype(np.float32)[None, :]
        vmem, hbm = pl.BlockSpec(memory_space=pltpu.VMEM), pl.BlockSpec(memory_space=pl.ANY)
        dma = pltpu.SemaphoreType.DMA
        cfg = (rows, early, seq, kv, hd, blk, nbuf, lag)
        k_part, v_part, o_part, lse, q_c, ke_c, ve_c = pl.pallas_call(
            functools.partial(stream_kernel, cfg),
            name='stream',
            out_shape=[jax.ShapeDtypeStruct(k_cache.shape, BF16), jax.ShapeDtypeStruct(v_cache.shape, BF16),
                       pltpu.VMEM((early * nq, hd), F32), pltpu.VMEM((nblk, 1, blk * nq), F32),
                       new_shape, new_shape, new_shape],
            in_specs=[pl.BlockSpec(memory_space=pltpu.SMEM), vmem, vmem, hbm, vmem, hbm, hbm, hbm, hbm, hbm],
            out_specs=[hbm, hbm, vmem, vmem, vmem, vmem, vmem],
            scratch_shapes=[
                pltpu.VMEM((rows, d_model), BF16),
                pltpu.VMEM(w_q.shape, BF16), pltpu.VMEM(w_k.shape, BF16), pltpu.VMEM(w_v.shape, BF16),
                pltpu.VMEM((2, rows, half), F32),
                pltpu.VMEM((2, early * nq, half), F32), pltpu.VMEM((2, early * kv, half), F32), pltpu.VMEM((2, early * kv, half), F32),
                pltpu.VMEM((nbuf, blk, seq, kv, hd), BF16), pltpu.VMEM((nbuf, blk, seq, kv, hd), BF16),
                pltpu.VMEM((blk * nq, 2 * seq * kv), BF16),
                dma((4,)), dma((nbuf,)), dma((nbuf,)), dma((nbuf,)), dma((nbuf,))],
            compiler_params=pltpu.CompilerParams(vmem_limit_bytes=56_000_000),
            cost_estimate=pl.CostEstimate(flops=10 ** 10, bytes_accessed=150_000_000, transcendentals=0),
        )(cur_pos, cur_pos.reshape(rows // 128, 128), inv_freq, x_in, w_pre, w_q, w_k, w_v, k_cache, v_cache)

        nc, d_f32 = 8, (8, d_model)
        late_shape = pltpu.VMEM((2, late) + k_cache.shape[1:], BF16)
        smem = pl.BlockSpec(memory_space=pltpu.SMEM)
        x_new, kv_late = pl.pallas_call(
            functools.partial(finish_kernel, (nc, nq, hd, early, blk)),
            name='finish',
            out_shape=[pltpu.VMEM(x_in.shape, BF16), late_shape],
            in_specs=[smem] + [vmem] * 5 + [hbm, vmem, hbm, hbm, hbm],
            out_specs=[vmem, vmem],
            scratch_shapes=[
                pltpu.VMEM((rows * nq, hd), F32), pltpu.VMEM((2 * nc, 1, 128), F32), pltpu.VMEM((blk * nq, 2 * seq * kv), BF16),
                pltpu.VMEM(x_in.shape, BF16),
                pltpu.VMEM(w_o.shape, BF16), pltpu.VMEM((nc, 128, hd), F32), pltpu.VMEM((2 * nc, 1, 128), F32),
                pltpu.VMEM((nc, hd // 128, 64, 128), F32), pltpu.VMEM((nc, 1, 128), F32),
                pltpu.VMEM((nc, hd // 128, 64, 128), F32), pltpu.VMEM((nc, 1, 128), F32),
                pltpu.VMEM((nc, hd // 128, 64, 128), F32), pltpu.VMEM((nc, 1, 128), F32),
                pltpu.VMEM((2, 128, 128), F32), pltpu.VMEM((hd // 128, 128, 128), F32),
                pltpu.VMEM((nc,) + d_f32, F32), pltpu.VMEM((nc,) + d_f32, F32), pltpu.VMEM((nc,) + d_f32, F32),
                pltpu.VMEM((8 * nc,) + d_f32, F32),
                dma((2,)), dma((2, late // blk))] + [dma((nc,))] * 18,
            compiler_params=pltpu.CompilerParams(vmem_limit_bytes=24_000_000, collective_id=0, has_side_effects=True),
            cost_estimate=pl.CostEstimate(flops=10 ** 10, bytes_accessed=100_000_000, transcendentals=0),
        )(cur_pos, o_part, lse, q_c, ke_c, ve_c, x_in, w_post, w_o, k_cache, v_cache)
        x_out, k_out, v_out, _ = pl.pallas_call(
            functools.partial(close_kernel, (early, blk, seq, nq, kv)),
            name='close',
            out_shape=[jax.ShapeDtypeStruct(x_in.shape, BF16), jax.ShapeDtypeStruct(k_cache.shape, BF16),
                       jax.ShapeDtypeStruct(v_cache.shape, BF16), late_shape],
            in_specs=[smem] + [vmem] * 4 + [hbm, hbm],
            out_specs=[hbm, hbm, hbm, vmem],
            input_output_aliases={4: 3, 5: 1, 6: 2},
            scratch_shapes=[dma, dma((2, late // blk))],
            compiler_params=pltpu.CompilerParams(vmem_limit_bytes=4_000_000),
        )(cur_pos, x_new, ke_c, ve_c, kv_late, k_part, v_part)
        return x_out, k_out, v_out

    return jax.shard_map(local_step, mesh=mesh,
                         in_specs=(P('dp', None), P('dp'), P(None), P(None, 'tp'), P(None, 'tp'), P(None, 'tp'), P('tp', None), P(None), cache_spec, cache_spec),
                         out_specs=(P('dp', None), cache_spec, cache_spec), check_vma=False)
```

```python
import functools

import jax
import jax.numpy as jnp
import numpy as np
from jax import lax
from jax.experimental import pallas as pl
from jax.experimental.pallas import tpu as pltpu
from jax.sharding import PartitionSpec as P

SOFT_CAP = 50.0
ROPE_BASE = 10000.0
NORM_EPS = 1e-6
NEG_FILL = -1e30
F32 = jnp.float32
BF16 = jnp.bfloat16


def rms_scale(tensor, gain_w):
    mean_sq = jnp.mean(tensor * tensor, axis=-1, keepdims=True)
    return tensor * lax.rsqrt(mean_sq + NORM_EPS) * (1.0 + gain_w)


def score_ids(nq, seq, kv, base):
    ng, width = nq * 2, 2 * seq * kv
    ri = lax.broadcasted_iota(jnp.int32, (ng, width), 0)
    ci = lax.broadcasted_iota(jnp.int32, (ng, width), 1)
    same = jnp.logical_and(ri // nq == ci // (seq * kv), (ri % nq) // (nq // kv) == ci % kv)
    return ng, width, ri < nq, jnp.where(same, (ci % (seq * kv)) // kv + base, 1 << 20)


def attend(k_of, v_of, q_of, lim_of, put, groups, ng, t_id, p_s, new=None):
    scale = k_of(0).shape[1] ** -0.5 / SOFT_CAP
    parts, hits = [], []
    if new is not None:
        q_lo, q_hi, k_lo, k_hi, v_lo, v_hi = new
        s_new = SOFT_CAP * jnp.tanh(jnp.sum(q_lo * k_lo + q_hi * k_hi, axis=-1, keepdims=True) * scale)
    for g in range(groups):
        s = lax.dot_general(q_of(g).astype(BF16), k_of(g), (((1,), (1,)), ((), ())), preferred_element_type=F32)
        s = SOFT_CAP * jnp.tanh(s * scale)
        lim = lim_of(g)
        if new is not None:
            hit = t_id == lim
            s = jnp.where(hit, s_new[g * ng:(g + 1) * ng, :], s)
            hits.append(jnp.where(hit, 1.0, 0.0))
        parts.append(jnp.where(t_id <= lim, s, NEG_FILL))
    sc = jnp.concatenate(parts, axis=0)
    m = jnp.max(sc, axis=-1, keepdims=True)
    e = jnp.where(sc > 0.5 * NEG_FILL, jnp.exp(sc - m), 0.0)
    l = jnp.sum(e, axis=-1, keepdims=True)
    some = l > 0.0
    inv = jnp.where(some, 1.0 / jnp.where(some, l, 1.0), 0.0)
    if new is not None:
        hit = jnp.concatenate(hits, axis=0)
        e_new = jnp.sum(e * hit, axis=-1, keepdims=True)
        e = e * (1.0 - hit)
        own = jnp.concatenate([v_lo * e_new, v_hi * e_new], axis=-1)
    p_s[...] = e.astype(BF16)
    for g in range(groups):
        r = slice(g * ng, (g + 1) * ng)
        o = jnp.dot(p_s[r, :], v_of(g), preferred_element_type=F32)
        if new is not None:
            o = o + own[r, :]
        put(g, o * inv[r, :])
    lse = jnp.where(some, m + jnp.log(jnp.where(some, l, 1.0)), NEG_FILL)
    return jnp.broadcast_to(lse, (groups * ng, 128)).T[0:1, :]


def stream_kernel(cfg, pos_s, pos_v, freq, x_hbm, gain, wq_hbm, wk_hbm, wv_hbm, kc, vc, k_out, v_out, o_ref, lse_ref, q_c, ke_c, ve_c,
                  a_v, wq_v, wk_v, wv_v, cs, q_s, kn_s, vn_s, kbuf, vbuf, p_s,
                  w_sem, kin, vin, kout, vout):
    rows, early, seq, kv, hd, blk, nbuf, lag = cfg
    late = rows - early
    nblk = early // blk
    groups = blk // 2
    half = hd // 2
    base = lax.axis_index('sp') * seq

    def k_in(j, s):
        return pltpu.make_async_copy(kc.at[pl.ds(j * blk, blk)], kbuf.at[s], kin.at[s])

    def v_in(j, s):
        return pltpu.make_async_copy(vc.at[pl.ds(j * blk, blk)], vbuf.at[s], vin.at[s])

    def k_o(j, s):
        return pltpu.make_async_copy(kbuf.at[s], k_out.at[pl.ds(j * blk, blk)], kout.at[s])

    def v_o(j, s):
        return pltpu.make_async_copy(vbuf.at[s], v_out.at[pl.ds(j * blk, blk)], vout.at[s])

    loads = [pltpu.make_async_copy(x_hbm, a_v, w_sem.at[0]), pltpu.make_async_copy(wq_hbm, wq_v, w_sem.at[1]),
             pltpu.make_async_copy(wk_hbm, wk_v, w_sem.at[2]), pltpu.make_async_copy(wv_hbm, wv_v, w_sem.at[3])]
    for c in loads:
        c.start()

    for i in range(rows // 128):
        ang = jnp.broadcast_to(pos_v[i:i + 1, :].astype(F32), (128, 128)).T * freq[...]
        cs[0, i * 128:(i + 1) * 128, :] = jnp.cos(ang)
        cs[1, i * 128:(i + 1) * 128, :] = jnp.sin(ang)

    loads[0].wait()
    step = 32

    @pl.loop(0, rows // step)
    def _(i):
        r = pl.ds(pl.multiple_of(i * step, step), step)
        a_v[r, :] = rms_scale(a_v[r, :].astype(F32), gain[...]).astype(BF16)

    for s in range(nbuf):
        k_in(s, s).start()
        v_in(s, s).start()

    nq = wq_v.shape[1] // hd

    def spread(pair, dst, h, stride, dst_c, heads):
        for i, part in enumerate(pair):
            part = part.astype(BF16).astype(F32)
            dst[i, pl.ds(h, early, stride=stride), :] = part[:early]
            for hc in heads:
                dst_c[i, pl.ds(hc, late, stride=nq), :] = part[early:]

    def rope(acc):
        lo, hi = acc[:, :half], acc[:, half:]
        return lo * cs[0] - hi * cs[1], hi * cs[0] + lo * cs[1]

    share = nq // kv
    loads[1].wait()
    for h in range(nq):
        acc = jnp.dot(a_v[...], wq_v[:, h * hd:(h + 1) * hd], preferred_element_type=F32)
        spread(rope(acc), q_s, h, nq, q_c, (h,))
    loads[2].wait()
    for h in range(kv):
        acc = jnp.dot(a_v[...], wk_v[:, h * hd:(h + 1) * hd], preferred_element_type=F32)
        spread(rope(acc), kn_s, h, kv, ke_c, range(h * share, (h + 1) * share))
    loads[3].wait()
    for h in range(kv):
        acc = jnp.dot(a_v[...], wv_v[:, h * hd:(h + 1) * hd], preferred_element_type=F32)
        spread((acc[:, :half], acc[:, half:]), vn_s, h, kv, ve_c, range(h * share, (h + 1) * share))

    ng, width, first, t_id = score_ids(nq, seq, kv, base)

    @pl.loop(0, nblk)
    def _(j):
        slot = lax.rem(j, nbuf)

        @pl.when(jnp.logical_and(j >= lag, j + nbuf - lag < nblk))
        def _():
            s2 = lax.rem(j - lag, nbuf)
            k_o(j - lag, s2).wait()
            k_in(j - lag + nbuf, s2).start()
            v_o(j - lag, s2).wait()
            v_in(j - lag + nbuf, s2).start()

        k_in(j, slot).wait()
        v_in(j, slot).wait()
        for i in range(blk):
            b = j * blk + i
            t = pos_s[b] - base
            hit = jnp.logical_and(t >= 0, t < seq)
            tt = jnp.clip(t, 0, seq - 1)
            r = pl.ds(kv * b, kv)
            row = jnp.concatenate([kn_s[0, r, :], kn_s[1, r, :]], axis=-1)
            kbuf[slot, i, tt] = jnp.where(hit, row, kbuf[slot, i, tt].astype(F32)).astype(BF16)
            row = jnp.concatenate([vn_s[0, r, :], vn_s[1, r, :]], axis=-1)
            vbuf[slot, i, tt] = jnp.where(hit, row, vbuf[slot, i, tt].astype(F32)).astype(BF16)

        def q_of(g):
            r = pl.ds(pl.multiple_of((j * groups + g) * ng, ng), ng)
            return jnp.concatenate([q_s[0, r, :], q_s[1, r, :]], axis=-1)

        def lim_of(g):
            return jnp.where(first, pos_s[j * blk + 2 * g], pos_s[j * blk + 2 * g + 1])

        def put(g, o):
            o_ref[pl.ds(pl.multiple_of((j * groups + g) * ng, ng), ng), :] = o

        lse_ref[j] = attend(lambda g: kbuf[slot, 2 * g:2 * g + 2].reshape(width, hd), lambda g: vbuf[slot, 2 * g:2 * g + 2].reshape(width, hd),
                            q_of, lim_of, put, groups, ng, t_id, p_s)
        k_o(j, slot).start()
        v_o(j, slot).start()

    for i in range(nbuf):
        j = nblk - nbuf + i
        k_o(j, j % nbuf).wait()
        v_o(j, j % nbuf).wait()


MESH_ID = pl.DeviceIdType.MESH


def merge_weights(a, b):
    top = jnp.maximum(a, b)
    ea, eb = jnp.exp(a - top), jnp.exp(b - top)
    tot = ea + eb
    return ea / tot, eb / tot, top + jnp.log(tot)


def columns(row):
    return jnp.broadcast_to(row, (128, 128)).T


def finish_kernel(cfg, pos_s, o_in, lse_in, q_c, ke_c, ve_c, x_hbm, gain, wo_hbm, kc, vc, out_ref, kv_buf,
                  o_ref, lse_ref, p_s, x_ref, wo_v, r1, r1l, k2, k2l, s2, s2l, r2, r2l, wt, tmp, su, ku, ru, gat,
                  l_sem, c_sem, s_d1, r_d1, s_dl, r_dl, s_x, r_x, s_xl, r_xl, s_y, r_y, s_ax, r_ax, s_ay, r_ay, s_f, r_f, s_d2, r_d2):
    nc, nq, hd, early, blk = cfg
    kbuf, vbuf = kv_buf.at[0], kv_buf.at[1]
    seq, kv = kc.shape[1], kc.shape[2]
    n_early, n_late = early // blk, kbuf.shape[0] // blk
    span = blk * nq
    dp, tp, sp = lax.axis_index('dp'), lax.axis_index('tp'), lax.axis_index('sp')
    core, xx = lax.rem(sp, 2), sp // 2
    partner = (dp, tp, xx * 2 + 1 - core)
    x_nbr = (dp, tp, (1 - xx) * 2 + core)
    y_nbr = (dp, 1 - tp, sp)

    def rcopy(src, dst, ss, rs, dev):
        return pltpu.make_async_remote_copy(src_ref=src, dst_ref=dst, send_sem=ss, recv_sem=rs, device_id=dev, device_id_type=MESH_ID)

    barrier = pltpu.get_barrier_semaphore()
    for dev in (partner, x_nbr, y_nbr):
        pl.semaphore_signal(barrier, inc=1, device_id=dev, device_id_type=MESH_ID)
    wo_load = pltpu.make_async_copy(wo_hbm, wo_v, l_sem.at[0])
    x_load = pltpu.make_async_copy(x_hbm, x_ref, l_sem.at[1])
    wo_load.start()
    x_load.start()

    def k_in(j):
        return pltpu.make_async_copy(kc.at[pl.ds(early + j * blk, blk)], kbuf.at[pl.ds(j * blk, blk)], c_sem.at[0, j])

    def v_in(j):
        return pltpu.make_async_copy(vc.at[pl.ds(early + j * blk, blk)], vbuf.at[pl.ds(j * blk, blk)], c_sem.at[1, j])

    @pl.loop(0, n_late)
    def _(j):
        k_in(j).start()
        v_in(j).start()

    @pl.loop(0, n_early)
    def _(j):
        r = pl.ds(pl.multiple_of(j * span, span), span)
        o_ref[r, :] = o_in[r, :]
        lse_ref[j] = lse_in[j]

    pl.semaphore_wait(barrier, 3)

    def d1(c):
        other = 2 * c + 1 - core
        return rcopy(o_ref.at[pl.ds(other * 128, 128)], r1.at[c], s_d1.at[c], r_d1.at[c], partner)

    def dl(c):
        other = 2 * c + 1 - core
        return rcopy(lse_ref.at[other], r1l.at[other], s_dl.at[c], r_dl.at[c], partner)

    def xs(c):
        return rcopy(s2.at[c], r2.at[c], s_x.at[c], r_x.at[c], x_nbr)

    def xl(c):
        return rcopy(s2l.at[c], r2l.at[c], s_xl.at[c], r_xl.at[c], x_nbr)

    def ys(c):
        return rcopy(su.at[c], ru.at[c], s_y.at[c], r_y.at[c], y_nbr)

    def slab(c, x, y):
        return c * 8 + core * 4 + x * 2 + y

    def ag(c, sems, rsems, dev):
        g = gat.at[slab(c, xx, tp)]
        return rcopy(g, g, sems.at[c], rsems.at[c], dev)

    def fw_y(c):
        g = gat.at[slab(c, 1 - xx, tp)]
        return rcopy(g, g, s_f.at[c], r_f.at[c], y_nbr)

    def fw_x(c):
        g = gat.at[slab(c, xx, 1 - tp)]
        return rcopy(g, g, s_f.at[c], r_f.at[c], x_nbr)

    def d2(c):
        g = gat.at[pl.ds(c * 8 + core * 4, 4)]
        return rcopy(g, g, s_d2.at[c], r_d2.at[c], partner)

    @pl.loop(0, n_early // 2)
    def _(c):
        dl(c).start()
        d1(c).start()

    ng, width, first, t_id = score_ids(nq, seq, kv, sp * seq)
    groups = blk // 2

    def stage_attend(j):
        k_in(j).wait()
        v_in(j).wait()
        rows = pl.ds(pl.multiple_of(j * span, span), span)
        at0 = pl.multiple_of(early * nq + j * span, span)
        new = (q_c[0, rows, :], q_c[1, rows, :], ke_c[0, rows, :], ke_c[1, rows, :], ve_c[0, rows, :], ve_c[1, rows, :])

        def q_of(g):
            r = pl.ds(pl.multiple_of(j * span + g * ng, ng), ng)
            return jnp.concatenate([q_c[0, r, :], q_c[1, r, :]], axis=-1)

        def lim_of(g):
            b = early + j * blk + 2 * g
            return jnp.where(first, pos_s[b], pos_s[b + 1])

        def put(g, o):
            o_ref[pl.ds(pl.multiple_of(at0 + g * ng, ng), ng), :] = o

        lse_ref[n_early + j] = attend(lambda g: kbuf[pl.ds(j * blk + 2 * g, 2)].reshape(width, hd),
                                      lambda g: vbuf[pl.ds(j * blk + 2 * g, 2)].reshape(width, hd),
                                      q_of, lim_of, put, groups, ng, t_id, p_s, new)

        @pl.when(lax.rem(j, 2) == 1)
        def _():
            c = (n_early + j) // 2
            dl(c).start()
            d1(c).start()

    def stage_a(c):
        d1(c).wait_recv()
        dl(c).wait_recv()
        mine = 2 * c + core
        wa, wb, lse = merge_weights(lse_ref[mine], r1l[mine])
        wa, wb = columns(wa), columns(wb)
        r = pl.ds(pl.multiple_of(mine * 128, 128), 128)
        for i in range(hd // 128):
            col = slice(i * 128, (i + 1) * 128)
            tmp[i] = o_ref[r, col] * wa + r1[c, :, col] * wb
            k2[c, i] = tmp[i, pl.ds(pl.multiple_of(xx * 64, 64), 64), :]
            s2[c, i] = tmp[i, pl.ds(pl.multiple_of((1 - xx) * 64, 64), 64), :]
        k2l[c] = lse
        s2l[c] = lse
        xs(c).start()
        xl(c).start()

    def stage_b(c):
        xs(c).wait_recv()
        xl(c).wait_recv()
        wa, wb, _ = merge_weights(k2l[c], r2l[c])
        wt[0] = columns(wa)
        wt[1] = columns(wb)
        r = pl.ds(pl.multiple_of(xx * 64, 64), 64)
        wa, wb = wt[0, r, :], wt[1, r, :]
        for i in range(hd // 128):
            tmp[i, 0:64, :] = k2[c, i] * wa + r2[c, i] * wb
        parts = [tmp[i, pl.ds(h, 16, stride=nq), :] for h in range(nq) for i in range(hd // 128)]
        attn = jnp.concatenate(parts, axis=-1).astype(BF16)
        d_model = wo_v.shape[1]
        for n in range(d_model // 256):
            col = slice(n * 256, (n + 1) * 256)
            u = jnp.dot(attn, wo_v[:, col], preferred_element_type=F32)
            ku[c, :, col] = jnp.where(tp == 0, u[:8], u[8:])
            su[c, :, col] = jnp.where(tp == 0, u[8:], u[:8])
        ys(c).start()

    def stage_c(c):
        ys(c).wait_recv()
        u = ku[c] + ru[c]
        x = x_ref[pl.ds(pl.multiple_of(c * 64 + core * 32 + xx * 16, 16), 16), :].astype(F32)
        x = jnp.where(tp == 0, x[:8], x[8:])
        gat[slab(c, xx, tp)] = x + rms_scale(u, gain[...])
        ag(c, s_ax, r_ax, x_nbr).start()
        ag(c, s_ay, r_ay, y_nbr).start()

    def stage_d(c):
        ag(c, s_ax, r_ax, x_nbr).wait_recv()
        ag(c, s_ay, r_ay, y_nbr).wait_recv()

        @pl.when(lax.rem(c, 3) != 2)
        def _():
            fw_x(c).start()

        @pl.when(lax.rem(c, 3) == 2)
        def _():
            fw_y(c).start()

    def stage_e(c):
        @pl.when(lax.rem(c, 3) != 2)
        def _():
            fw_x(c).wait_recv()

        @pl.when(lax.rem(c, 3) == 2)
        def _():
            fw_y(c).wait_recv()

        d2(c).start()

    def stage_f(c):
        d2(c).wait_recv()
        for i in range(4):
            both = gat[pl.ds(c * 8 + 2 * i, 2)]
            out_ref[pl.ds(pl.multiple_of(c * 64 + 16 * i, 16), 16), :] = both.reshape(16, both.shape[-1]).astype(BF16)

    def at(t, lag, stage):
        c = t - lag

        @pl.when(jnp.logical_and(c >= 0, c < nc))
        def _():
            stage(c)

    @pl.loop(0, nc + 9)
    def _(t):
        at(t, 4, stage_c)
        at(t, 6, stage_d)
        at(t, 0, stage_a)

        @pl.when(t == 2)
        def _():
            wo_load.wait()
            x_load.wait()

        at(t, 2, stage_b)
        at(t, 8, stage_e)
        at(t, 9, stage_f)

        @pl.when(jnp.logical_and(t >= 1, t <= n_late))
        def _():
            stage_attend(t - 1)

    @pl.loop(0, nc)
    def _(c):
        d1(c).wait_send()
        dl(c).wait_send()
        xs(c).wait_send()
        xl(c).wait_send()
        ys(c).wait_send()
        ag(c, s_ax, r_ax, x_nbr).wait_send()
        ag(c, s_ay, r_ay, y_nbr).wait_send()
        fw_x(c).wait_send()
        d2(c).wait_send()


def close_kernel(cfg, pos_s, x_ref, ke_c, ve_c, kv_in, k_part, v_part, x_out, k_out, v_out, kv_buf, x_sem, o_sem):
    kb, vb = kv_buf.at[0], kv_buf.at[1]
    early, blk, seq, nq, kv = cfg
    base = lax.axis_index('sp') * seq
    n_late = kb.shape[0] // blk
    copy = pltpu.make_async_copy(x_ref, x_out, x_sem)
    copy.start()

    def out(i, buf, dst, j):
        return pltpu.make_async_copy(buf.at[pl.ds(j * blk, blk)], dst.at[pl.ds(early + j * blk, blk)], o_sem.at[i, j])

    @pl.loop(0, n_late)
    def _(j):
        for i in range(blk):
            b = j * blk + i
            t = pos_s[early + b] - base
            hit = jnp.logical_and(t >= 0, t < seq)
            tt = jnp.clip(t, 0, seq - 1)
            r = pl.ds(nq * b, kv, stride=nq // kv)
            for buf, new in ((kb, ke_c), (vb, ve_c)):
                row = jnp.concatenate([new[0, r, :], new[1, r, :]], axis=-1)
                buf[b, tt] = jnp.where(hit, row, buf[b, tt].astype(F32)).astype(BF16)
        out(0, kb, k_out, j).start()
        out(1, vb, v_out, j).start()

    @pl.loop(0, n_late)
    def _(j):
        out(0, kb, k_out, j).wait()
        out(1, vb, v_out, j).wait()

    copy.wait()


def solution(mesh):
    cache_spec = P('dp', 'sp', 'tp', None)

    def local_step(x_in, cur_pos, w_pre, w_q, w_k, w_v, w_o, w_post, k_cache, v_cache):
        rows, seq, kv, hd = k_cache.shape
        d_model = x_in.shape[1]
        nq = w_q.shape[1] // hd
        half = hd // 2
        blk, nbuf, lag = 32, 8, 3
        late = 192
        early = rows - late
        nblk = early // blk
        new_shape = pltpu.VMEM((2, late * nq, half), F32)
        inv_freq = (ROPE_BASE ** (-2.0 * np.arange(half) / hd)).astype(np.float32)[None, :]
        vmem, hbm = pl.BlockSpec(memory_space=pltpu.VMEM), pl.BlockSpec(memory_space=pl.ANY)
        dma = pltpu.SemaphoreType.DMA
        cfg = (rows, early, seq, kv, hd, blk, nbuf, lag)
        k_part, v_part, o_part, lse, q_c, ke_c, ve_c = pl.pallas_call(
            functools.partial(stream_kernel, cfg),
            name='stream',
            out_shape=[jax.ShapeDtypeStruct(k_cache.shape, BF16), jax.ShapeDtypeStruct(v_cache.shape, BF16),
                       pltpu.VMEM((early * nq, hd), F32), pltpu.VMEM((nblk, 1, blk * nq), F32),
                       new_shape, new_shape, new_shape],
            in_specs=[pl.BlockSpec(memory_space=pltpu.SMEM), vmem, vmem, hbm, vmem, hbm, hbm, hbm, hbm, hbm],
            out_specs=[hbm, hbm, vmem, vmem, vmem, vmem, vmem],
            scratch_shapes=[
                pltpu.VMEM((rows, d_model), BF16),
                pltpu.VMEM(w_q.shape, BF16), pltpu.VMEM(w_k.shape, BF16), pltpu.VMEM(w_v.shape, BF16),
                pltpu.VMEM((2, rows, half), F32),
                pltpu.VMEM((2, early * nq, half), F32), pltpu.VMEM((2, early * kv, half), F32), pltpu.VMEM((2, early * kv, half), F32),
                pltpu.VMEM((nbuf, blk, seq, kv, hd), BF16), pltpu.VMEM((nbuf, blk, seq, kv, hd), BF16),
                pltpu.VMEM((blk * nq, 2 * seq * kv), BF16),
                dma((4,)), dma((nbuf,)), dma((nbuf,)), dma((nbuf,)), dma((nbuf,))],
            compiler_params=pltpu.CompilerParams(vmem_limit_bytes=56_000_000),
            cost_estimate=pl.CostEstimate(flops=10 ** 10, bytes_accessed=150_000_000, transcendentals=0),
        )(cur_pos, cur_pos.reshape(rows // 128, 128), inv_freq, x_in, w_pre, w_q, w_k, w_v, k_cache, v_cache)

        nc, d_f32 = 8, (8, d_model)
        late_shape = pltpu.VMEM((2, late) + k_cache.shape[1:], BF16)
        smem = pl.BlockSpec(memory_space=pltpu.SMEM)
        x_new, kv_late = pl.pallas_call(
            functools.partial(finish_kernel, (nc, nq, hd, early, blk)),
            name='finish',
            out_shape=[pltpu.VMEM(x_in.shape, BF16), late_shape],
            in_specs=[smem] + [vmem] * 5 + [hbm, vmem, hbm, hbm, hbm],
            out_specs=[vmem, vmem],
            scratch_shapes=[
                pltpu.VMEM((rows * nq, hd), F32), pltpu.VMEM((2 * nc, 1, 128), F32), pltpu.VMEM((blk * nq, 2 * seq * kv), BF16),
                pltpu.VMEM(x_in.shape, BF16),
                pltpu.VMEM(w_o.shape, BF16), pltpu.VMEM((nc, 128, hd), F32), pltpu.VMEM((2 * nc, 1, 128), F32),
                pltpu.VMEM((nc, hd // 128, 64, 128), F32), pltpu.VMEM((nc, 1, 128), F32),
                pltpu.VMEM((nc, hd // 128, 64, 128), F32), pltpu.VMEM((nc, 1, 128), F32),
                pltpu.VMEM((nc, hd // 128, 64, 128), F32), pltpu.VMEM((nc, 1, 128), F32),
                pltpu.VMEM((2, 128, 128), F32), pltpu.VMEM((hd // 128, 128, 128), F32),
                pltpu.VMEM((nc,) + d_f32, F32), pltpu.VMEM((nc,) + d_f32, F32), pltpu.VMEM((nc,) + d_f32, F32),
                pltpu.VMEM((8 * nc,) + d_f32, F32),
                dma((2,)), dma((2, late // blk))] + [dma((nc,))] * 18,
            compiler_params=pltpu.CompilerParams(vmem_limit_bytes=24_000_000, collective_id=0, has_side_effects=True),
            cost_estimate=pl.CostEstimate(flops=10 ** 10, bytes_accessed=100_000_000, transcendentals=0),
        )(cur_pos, o_part, lse, q_c, ke_c, ve_c, x_in, w_post, w_o, k_cache, v_cache)
        x_out, k_out, v_out, _ = pl.pallas_call(
            functools.partial(close_kernel, (early, blk, seq, nq, kv)),
            name='close',
            out_shape=[jax.ShapeDtypeStruct(x_in.shape, BF16), jax.ShapeDtypeStruct(k_cache.shape, BF16),
                       jax.ShapeDtypeStruct(v_cache.shape, BF16), late_shape],
            in_specs=[smem] + [vmem] * 4 + [hbm, hbm],
            out_specs=[hbm, hbm, hbm, vmem],
            input_output_aliases={4: 3, 5: 1, 6: 2},
            scratch_shapes=[dma, dma((2, late // blk))],
            compiler_params=pltpu.CompilerParams(vmem_limit_bytes=4_000_000),
        )(cur_pos, x_new, ke_c, ve_c, kv_late, k_part, v_part)
        return x_out, k_out, v_out

    return jax.shard_map(local_step, mesh=mesh,
                         in_specs=(P('dp', None), P('dp'), P(None), P(None, 'tp'), P(None, 'tp'), P(None, 'tp'), P('tp', None), P(None), cache_spec, cache_spec),
                         out_specs=(P('dp', None), cache_spec, cache_spec), check_vma=False)
```

```python
import functools

import jax
import jax.numpy as jnp
import numpy as np
from jax import lax
from jax.experimental import pallas as pl
from jax.experimental.pallas import tpu as pltpu
from jax.sharding import PartitionSpec as P

SOFT_CAP = 50.0
ROPE_BASE = 10000.0
NORM_EPS = 1e-6
NEG_FILL = -1e30
F32 = jnp.float32
BF16 = jnp.bfloat16


def rms_scale(tensor, gain_w):
    mean_sq = jnp.mean(tensor * tensor, axis=-1, keepdims=True)
    return tensor * lax.rsqrt(mean_sq + NORM_EPS) * (1.0 + gain_w)


def score_ids(nq, seq, kv, base):
    ng, width = nq * 2, 2 * seq * kv
    ri = lax.broadcasted_iota(jnp.int32, (ng, width), 0)
    ci = lax.broadcasted_iota(jnp.int32, (ng, width), 1)
    same = jnp.logical_and(ri // nq == ci // (seq * kv), (ri % nq) // (nq // kv) == ci % kv)
    return ng, width, ri < nq, jnp.where(same, (ci % (seq * kv)) // kv + base, 1 << 20)


def attend(k_of, v_of, q_of, lim_of, put, groups, ng, t_id, p_s, new=None):
    scale = k_of(0).shape[1] ** -0.5 / SOFT_CAP
    parts, hits = [], []
    if new is not None:
        q_lo, q_hi, k_lo, k_hi, v_lo, v_hi = new
        s_new = SOFT_CAP * jnp.tanh(jnp.sum(q_lo * k_lo + q_hi * k_hi, axis=-1, keepdims=True) * scale)
    for g in range(groups):
        s = lax.dot_general(q_of(g).astype(BF16), k_of(g), (((1,), (1,)), ((), ())), preferred_element_type=F32)
        s = SOFT_CAP * jnp.tanh(s * scale)
        lim = lim_of(g)
        if new is not None:
            hit = t_id == lim
            s = jnp.where(hit, s_new[g * ng:(g + 1) * ng, :], s)
            hits.append(jnp.where(hit, 1.0, 0.0))
        parts.append(jnp.where(t_id <= lim, s, NEG_FILL))
    sc = jnp.concatenate(parts, axis=0)
    m = jnp.max(sc, axis=-1, keepdims=True)
    e = jnp.where(sc > 0.5 * NEG_FILL, jnp.exp(sc - m), 0.0)
    l = jnp.sum(e, axis=-1, keepdims=True)
    some = l > 0.0
    inv = jnp.where(some, 1.0 / jnp.where(some, l, 1.0), 0.0)
    if new is not None:
        hit = jnp.concatenate(hits, axis=0)
        e_new = jnp.sum(e * hit, axis=-1, keepdims=True)
        e = e * (1.0 - hit)
        own = jnp.concatenate([v_lo * e_new, v_hi * e_new], axis=-1)
    p_s[...] = e.astype(BF16)
    for g in range(groups):
        r = slice(g * ng, (g + 1) * ng)
        o = jnp.dot(p_s[r, :], v_of(g), preferred_element_type=F32)
        if new is not None:
            o = o + own[r, :]
        put(g, o * inv[r, :])
    lse = jnp.where(some, m + jnp.log(jnp.where(some, l, 1.0)), NEG_FILL)
    return jnp.broadcast_to(lse, (groups * ng, 128)).T[0:1, :]


def stream_kernel(cfg, pos_s, pos_v, freq, x_hbm, gain, wq_hbm, wk_hbm, wv_hbm, kc, vc, k_out, v_out, o_ref, lse_ref, q_c, ke_c, ve_c,
                  a_v, wq_v, wk_v, wv_v, cs, q_s, kn_s, vn_s, kbuf, vbuf, p_s,
                  w_sem, kin, vin, kout, vout):
    rows, early, seq, kv, hd, blk, nbuf, lag = cfg
    late = rows - early
    nblk = early // blk
    groups = blk // 2
    half = hd // 2
    base = lax.axis_index('sp') * seq

    def k_in(j, s):
        return pltpu.make_async_copy(kc.at[pl.ds(j * blk, blk)], kbuf.at[s], kin.at[s])

    def v_in(j, s):
        return pltpu.make_async_copy(vc.at[pl.ds(j * blk, blk)], vbuf.at[s], vin.at[s])

    def k_o(j, s):
        return pltpu.make_async_copy(kbuf.at[s], k_out.at[pl.ds(j * blk, blk)], kout.at[s])

    def v_o(j, s):
        return pltpu.make_async_copy(vbuf.at[s], v_out.at[pl.ds(j * blk, blk)], vout.at[s])

    loads = [pltpu.make_async_copy(x_hbm, a_v, w_sem.at[0]), pltpu.make_async_copy(wq_hbm, wq_v, w_sem.at[1]),
             pltpu.make_async_copy(wk_hbm, wk_v, w_sem.at[2]), pltpu.make_async_copy(wv_hbm, wv_v, w_sem.at[3])]
    for c in loads:
        c.start()

    for i in range(rows // 128):
        ang = jnp.broadcast_to(pos_v[i:i + 1, :].astype(F32), (128, 128)).T * freq[...]
        cs[0, i * 128:(i + 1) * 128, :] = jnp.cos(ang)
        cs[1, i * 128:(i + 1) * 128, :] = jnp.sin(ang)

    loads[0].wait()
    step = 32

    @pl.loop(0, rows // step)
    def _(i):
        r = pl.ds(pl.multiple_of(i * step, step), step)
        a_v[r, :] = rms_scale(a_v[r, :].astype(F32), gain[...]).astype(BF16)

    for s in range(nbuf):
        k_in(s, s).start()
        v_in(s, s).start()

    nq = wq_v.shape[1] // hd

    def spread(pair, dst, h, stride, dst_c, heads):
        for i, part in enumerate(pair):
            part = part.astype(BF16).astype(F32)
            dst[i, pl.ds(h, early, stride=stride), :] = part[:early]
            for hc in heads:
                dst_c[i, pl.ds(hc, late, stride=nq), :] = part[early:]

    def rope(acc):
        lo, hi = acc[:, :half], acc[:, half:]
        return lo * cs[0] - hi * cs[1], hi * cs[0] + lo * cs[1]

    share = nq // kv
    loads[1].wait()
    for h in range(nq):
        acc = jnp.dot(a_v[...], wq_v[:, h * hd:(h + 1) * hd], preferred_element_type=F32)
        spread(rope(acc), q_s, h, nq, q_c, (h,))
    loads[2].wait()
    for h in range(kv):
        acc = jnp.dot(a_v[...], wk_v[:, h * hd:(h + 1) * hd], preferred_element_type=F32)
        spread(rope(acc), kn_s, h, kv, ke_c, range(h * share, (h + 1) * share))
    loads[3].wait()
    for h in range(kv):
        acc = jnp.dot(a_v[...], wv_v[:, h * hd:(h + 1) * hd], preferred_element_type=F32)
        spread((acc[:, :half], acc[:, half:]), vn_s, h, kv, ve_c, range(h * share, (h + 1) * share))

    ng, width, first, t_id = score_ids(nq, seq, kv, base)

    @pl.loop(0, nblk)
    def _(j):
        slot = lax.rem(j, nbuf)

        @pl.when(jnp.logical_and(j >= lag, j + nbuf - lag < nblk))
        def _():
            s2 = lax.rem(j - lag, nbuf)
            k_o(j - lag, s2).wait()
            k_in(j - lag + nbuf, s2).start()
            v_o(j - lag, s2).wait()
            v_in(j - lag + nbuf, s2).start()

        k_in(j, slot).wait()
        v_in(j, slot).wait()
        for i in range(blk):
            b = j * blk + i
            t = pos_s[b] - base
            hit = jnp.logical_and(t >= 0, t < seq)
            tt = jnp.clip(t, 0, seq - 1)
            r = pl.ds(kv * b, kv)
            row = jnp.concatenate([kn_s[0, r, :], kn_s[1, r, :]], axis=-1)
            kbuf[slot, i, tt] = jnp.where(hit, row, kbuf[slot, i, tt].astype(F32)).astype(BF16)
            row = jnp.concatenate([vn_s[0, r, :], vn_s[1, r, :]], axis=-1)
            vbuf[slot, i, tt] = jnp.where(hit, row, vbuf[slot, i, tt].astype(F32)).astype(BF16)

        def q_of(g):
            r = pl.ds(pl.multiple_of((j * groups + g) * ng, ng), ng)
            return jnp.concatenate([q_s[0, r, :], q_s[1, r, :]], axis=-1)

        def lim_of(g):
            return jnp.where(first, pos_s[j * blk + 2 * g], pos_s[j * blk + 2 * g + 1])

        def put(g, o):
            o_ref[pl.ds(pl.multiple_of((j * groups + g) * ng, ng), ng), :] = o

        lse_ref[j] = attend(lambda g: kbuf[slot, 2 * g:2 * g + 2].reshape(width, hd), lambda g: vbuf[slot, 2 * g:2 * g + 2].reshape(width, hd),
                            q_of, lim_of, put, groups, ng, t_id, p_s)
        k_o(j, slot).start()
        v_o(j, slot).start()

    for i in range(nbuf):
        j = nblk - nbuf + i
        k_o(j, j % nbuf).wait()
        v_o(j, j % nbuf).wait()


MESH_ID = pl.DeviceIdType.MESH


def merge_weights(a, b):
    top = jnp.maximum(a, b)
    ea, eb = jnp.exp(a - top), jnp.exp(b - top)
    tot = ea + eb
    return ea / tot, eb / tot, top + jnp.log(tot)


def columns(row):
    return jnp.broadcast_to(row, (128, 128)).T


def finish_kernel(cfg, pos_s, o_in, lse_in, q_c, ke_c, ve_c, x_hbm, gain, wo_hbm, kc, vc, out_ref, kv_buf,
                  o_ref, lse_ref, p_s, x_ref, wo_v, r1, r1l, k2, k2l, s2, s2l, r2, r2l, wt, tmp, su, ku, ru, gat,
                  l_sem, c_sem, s_d1, r_d1, s_dl, r_dl, s_x, r_x, s_xl, r_xl, s_y, r_y, s_ax, r_ax, s_ay, r_ay, s_f, r_f, s_d2, r_d2):
    nc, nq, hd, early, blk = cfg
    kbuf, vbuf = kv_buf.at[0], kv_buf.at[1]
    seq, kv = kc.shape[1], kc.shape[2]
    n_early, n_late = early // blk, kbuf.shape[0] // blk
    span = blk * nq
    dp, tp, sp = lax.axis_index('dp'), lax.axis_index('tp'), lax.axis_index('sp')
    core, xx = lax.rem(sp, 2), sp // 2
    partner = (dp, tp, xx * 2 + 1 - core)
    x_nbr = (dp, tp, (1 - xx) * 2 + core)
    y_nbr = (dp, 1 - tp, sp)

    def rcopy(src, dst, ss, rs, dev):
        return pltpu.make_async_remote_copy(src_ref=src, dst_ref=dst, send_sem=ss, recv_sem=rs, device_id=dev, device_id_type=MESH_ID)

    barrier = pltpu.get_barrier_semaphore()
    for dev in (partner, x_nbr, y_nbr):
        pl.semaphore_signal(barrier, inc=1, device_id=dev, device_id_type=MESH_ID)
    wo_load = pltpu.make_async_copy(wo_hbm, wo_v, l_sem.at[0])
    x_load = pltpu.make_async_copy(x_hbm, x_ref, l_sem.at[1])
    wo_load.start()
    x_load.start()

    def k_in(j):
        return pltpu.make_async_copy(kc.at[pl.ds(early + j * blk, blk)], kbuf.at[pl.ds(j * blk, blk)], c_sem.at[0, j])

    def v_in(j):
        return pltpu.make_async_copy(vc.at[pl.ds(early + j * blk, blk)], vbuf.at[pl.ds(j * blk, blk)], c_sem.at[1, j])

    @pl.loop(0, n_late)
    def _(j):
        k_in(j).start()
        v_in(j).start()

    @pl.loop(0, n_early)
    def _(j):
        r = pl.ds(pl.multiple_of(j * span, span), span)
        o_ref[r, :] = o_in[r, :]
        lse_ref[j] = lse_in[j]

    pl.semaphore_wait(barrier, 3)

    def d1(c):
        other = 2 * c + 1 - core
        return rcopy(o_ref.at[pl.ds(other * 128, 128)], r1.at[c], s_d1.at[c], r_d1.at[c], partner)

    def dl(c):
        other = 2 * c + 1 - core
        return rcopy(lse_ref.at[other], r1l.at[other], s_dl.at[c], r_dl.at[c], partner)

    def xs(c):
        return rcopy(s2.at[c], r2.at[c], s_x.at[c], r_x.at[c], x_nbr)

    def xl(c):
        return rcopy(s2l.at[c], r2l.at[c], s_xl.at[c], r_xl.at[c], x_nbr)

    def ys(c):
        return rcopy(su.at[c], ru.at[c], s_y.at[c], r_y.at[c], y_nbr)

    def slab(c, x, y):
        return c * 8 + core * 4 + x * 2 + y

    def ag(c, sems, rsems, dev):
        g = gat.at[slab(c, xx, tp)]
        return rcopy(g, g, sems.at[c], rsems.at[c], dev)

    def fw_y(c):
        g = gat.at[slab(c, 1 - xx, tp)]
        return rcopy(g, g, s_f.at[c], r_f.at[c], y_nbr)

    def fw_x(c):
        g = gat.at[slab(c, xx, 1 - tp)]
        return rcopy(g, g, s_f.at[c], r_f.at[c], x_nbr)

    def d2(c):
        g = gat.at[pl.ds(c * 8 + core * 4, 4)]
        return rcopy(g, g, s_d2.at[c], r_d2.at[c], partner)

    @pl.loop(0, n_early // 2)
    def _(c):
        dl(c).start()
        d1(c).start()

    ng, width, first, t_id = score_ids(nq, seq, kv, sp * seq)
    groups = blk // 2

    def stage_attend(j):
        k_in(j).wait()
        v_in(j).wait()
        rows = pl.ds(pl.multiple_of(j * span, span), span)
        at0 = pl.multiple_of(early * nq + j * span, span)
        new = (q_c[0, rows, :], q_c[1, rows, :], ke_c[0, rows, :], ke_c[1, rows, :], ve_c[0, rows, :], ve_c[1, rows, :])

        def q_of(g):
            r = pl.ds(pl.multiple_of(j * span + g * ng, ng), ng)
            return jnp.concatenate([q_c[0, r, :], q_c[1, r, :]], axis=-1)

        def lim_of(g):
            b = early + j * blk + 2 * g
            return jnp.where(first, pos_s[b], pos_s[b + 1])

        def put(g, o):
            o_ref[pl.ds(pl.multiple_of(at0 + g * ng, ng), ng), :] = o

        lse_ref[n_early + j] = attend(lambda g: kbuf[pl.ds(j * blk + 2 * g, 2)].reshape(width, hd),
                                      lambda g: vbuf[pl.ds(j * blk + 2 * g, 2)].reshape(width, hd),
                                      q_of, lim_of, put, groups, ng, t_id, p_s, new)

        @pl.when(lax.rem(j, 2) == 1)
        def _():
            c = (n_early + j) // 2
            dl(c).start()
            d1(c).start()

    def stage_a(c):
        d1(c).wait_recv()
        dl(c).wait_recv()
        mine = 2 * c + core
        wa, wb, lse = merge_weights(lse_ref[mine], r1l[mine])
        wa, wb = columns(wa), columns(wb)
        r = pl.ds(pl.multiple_of(mine * 128, 128), 128)
        for i in range(hd // 128):
            col = slice(i * 128, (i + 1) * 128)
            tmp[i] = o_ref[r, col] * wa + r1[c, :, col] * wb
            k2[c, i] = tmp[i, pl.ds(pl.multiple_of(xx * 64, 64), 64), :]
            s2[c, i] = tmp[i, pl.ds(pl.multiple_of((1 - xx) * 64, 64), 64), :]
        k2l[c] = lse
        s2l[c] = lse
        xs(c).start()
        xl(c).start()

    def stage_b(c):
        xs(c).wait_recv()
        xl(c).wait_recv()
        wa, wb, _ = merge_weights(k2l[c], r2l[c])
        wt[0] = columns(wa)
        wt[1] = columns(wb)
        r = pl.ds(pl.multiple_of(xx * 64, 64), 64)
        wa, wb = wt[0, r, :], wt[1, r, :]
        for i in range(hd // 128):
            tmp[i, 0:64, :] = k2[c, i] * wa + r2[c, i] * wb
        parts = [tmp[i, pl.ds(h, 16, stride=nq), :] for h in range(nq) for i in range(hd // 128)]
        attn = jnp.concatenate(parts, axis=-1).astype(BF16)
        d_model = wo_v.shape[1]
        for n in range(d_model // 256):
            col = slice(n * 256, (n + 1) * 256)
            u = jnp.dot(attn, wo_v[:, col], preferred_element_type=F32)
            ku[c, :, col] = jnp.where(tp == 0, u[:8], u[8:])
            su[c, :, col] = jnp.where(tp == 0, u[8:], u[:8])
        ys(c).start()

    def stage_c(c):
        ys(c).wait_recv()
        u = ku[c] + ru[c]
        x = x_ref[pl.ds(pl.multiple_of(c * 64 + core * 32 + xx * 16, 16), 16), :].astype(F32)
        x = jnp.where(tp == 0, x[:8], x[8:])
        gat[slab(c, xx, tp)] = x + rms_scale(u, gain[...])
        ag(c, s_ax, r_ax, x_nbr).start()
        ag(c, s_ay, r_ay, y_nbr).start()

    def stage_d(c):
        ag(c, s_ax, r_ax, x_nbr).wait_recv()
        ag(c, s_ay, r_ay, y_nbr).wait_recv()

        @pl.when(lax.rem(c, 3) != 2)
        def _():
            fw_x(c).start()

        @pl.when(lax.rem(c, 3) == 2)
        def _():
            fw_y(c).start()

    def stage_e(c):
        @pl.when(lax.rem(c, 3) != 2)
        def _():
            fw_x(c).wait_recv()

        @pl.when(lax.rem(c, 3) == 2)
        def _():
            fw_y(c).wait_recv()

        d2(c).start()

    def stage_f(c):
        d2(c).wait_recv()
        for i in range(4):
            both = gat[pl.ds(c * 8 + 2 * i, 2)]
            out_ref[pl.ds(pl.multiple_of(c * 64 + 16 * i, 16), 16), :] = both.reshape(16, both.shape[-1]).astype(BF16)

    def at(t, lag, stage):
        c = t - lag

        @pl.when(jnp.logical_and(c >= 0, c < nc))
        def _():
            stage(c)

    @pl.loop(0, nc + 9)
    def _(t):
        at(t, 4, stage_c)
        at(t, 6, stage_d)
        at(t, 0, stage_a)

        @pl.when(t == 2)
        def _():
            wo_load.wait()
            x_load.wait()

        at(t, 2, stage_b)
        at(t, 8, stage_e)
        at(t, 9, stage_f)

        @pl.when(jnp.logical_and(t >= 1, t <= n_late))
        def _():
            stage_attend(t - 1)

    @pl.loop(0, nc)
    def _(c):
        d1(c).wait_send()
        dl(c).wait_send()
        xs(c).wait_send()
        xl(c).wait_send()
        ys(c).wait_send()
        ag(c, s_ax, r_ax, x_nbr).wait_send()
        ag(c, s_ay, r_ay, y_nbr).wait_send()
        fw_x(c).wait_send()
        d2(c).wait_send()


def close_kernel(cfg, pos_s, x_ref, ke_c, ve_c, kv_in, k_part, v_part, x_out, k_out, v_out, kv_buf, x_sem, o_sem):
    kb, vb = kv_buf.at[0], kv_buf.at[1]
    early, blk, seq, nq, kv = cfg
    base = lax.axis_index('sp') * seq
    n_late = kb.shape[0] // blk
    copy = pltpu.make_async_copy(x_ref, x_out, x_sem)
    copy.start()

    def out(i, buf, dst, j):
        return pltpu.make_async_copy(buf.at[pl.ds(j * blk, blk)], dst.at[pl.ds(early + j * blk, blk)], o_sem.at[i, j])

    @pl.loop(0, n_late)
    def _(j):
        for i in range(blk):
            b = j * blk + i
            t = pos_s[early + b] - base
            hit = jnp.logical_and(t >= 0, t < seq)
            tt = jnp.clip(t, 0, seq - 1)
            r = pl.ds(nq * b, kv, stride=nq // kv)
            for buf, new in ((kb, ke_c), (vb, ve_c)):
                row = jnp.concatenate([new[0, r, :], new[1, r, :]], axis=-1)
                buf[b, tt] = jnp.where(hit, row, buf[b, tt].astype(F32)).astype(BF16)
        out(0, kb, k_out, j).start()
        out(1, vb, v_out, j).start()

    @pl.loop(0, n_late)
    def _(j):
        out(0, kb, k_out, j).wait()
        out(1, vb, v_out, j).wait()

    copy.wait()


def solution(mesh):
    cache_spec = P('dp', 'sp', 'tp', None)

    def local_step(x_in, cur_pos, w_pre, w_q, w_k, w_v, w_o, w_post, k_cache, v_cache):
        rows, seq, kv, hd = k_cache.shape
        d_model = x_in.shape[1]
        nq = w_q.shape[1] // hd
        half = hd // 2
        blk, nbuf, lag = 32, 8, 2
        late = 192
        early = rows - late
        nblk = early // blk
        new_shape = pltpu.VMEM((2, late * nq, half), F32)
        inv_freq = (ROPE_BASE ** (-2.0 * np.arange(half) / hd)).astype(np.float32)[None, :]
        vmem, hbm = pl.BlockSpec(memory_space=pltpu.VMEM), pl.BlockSpec(memory_space=pl.ANY)
        dma = pltpu.SemaphoreType.DMA
        cfg = (rows, early, seq, kv, hd, blk, nbuf, lag)
        k_part, v_part, o_part, lse, q_c, ke_c, ve_c = pl.pallas_call(
            functools.partial(stream_kernel, cfg),
            name='stream',
            out_shape=[jax.ShapeDtypeStruct(k_cache.shape, BF16), jax.ShapeDtypeStruct(v_cache.shape, BF16),
                       pltpu.VMEM((early * nq, hd), F32), pltpu.VMEM((nblk, 1, blk * nq), F32),
                       new_shape, new_shape, new_shape],
            in_specs=[pl.BlockSpec(memory_space=pltpu.SMEM), vmem, vmem, hbm, vmem, hbm, hbm, hbm, hbm, hbm],
            out_specs=[hbm, hbm, vmem, vmem, vmem, vmem, vmem],
            scratch_shapes=[
                pltpu.VMEM((rows, d_model), BF16),
                pltpu.VMEM(w_q.shape, BF16), pltpu.VMEM(w_k.shape, BF16), pltpu.VMEM(w_v.shape, BF16),
                pltpu.VMEM((2, rows, half), F32),
                pltpu.VMEM((2, early * nq, half), F32), pltpu.VMEM((2, early * kv, half), F32), pltpu.VMEM((2, early * kv, half), F32),
                pltpu.VMEM((nbuf, blk, seq, kv, hd), BF16), pltpu.VMEM((nbuf, blk, seq, kv, hd), BF16),
                pltpu.VMEM((blk * nq, 2 * seq * kv), BF16),
                dma((4,)), dma((nbuf,)), dma((nbuf,)), dma((nbuf,)), dma((nbuf,))],
            compiler_params=pltpu.CompilerParams(vmem_limit_bytes=56_000_000),
            cost_estimate=pl.CostEstimate(flops=10 ** 10, bytes_accessed=150_000_000, transcendentals=0),
        )(cur_pos, cur_pos.reshape(rows // 128, 128), inv_freq, x_in, w_pre, w_q, w_k, w_v, k_cache, v_cache)

        nc, d_f32 = 8, (8, d_model)
        late_shape = pltpu.VMEM((2, late) + k_cache.shape[1:], BF16)
        smem = pl.BlockSpec(memory_space=pltpu.SMEM)
        x_new, kv_late = pl.pallas_call(
            functools.partial(finish_kernel, (nc, nq, hd, early, blk)),
            name='finish',
            out_shape=[pltpu.VMEM(x_in.shape, BF16), late_shape],
            in_specs=[smem] + [vmem] * 5 + [hbm, vmem, hbm, hbm, hbm],
            out_specs=[vmem, vmem],
            scratch_shapes=[
                pltpu.VMEM((rows * nq, hd), F32), pltpu.VMEM((2 * nc, 1, 128), F32), pltpu.VMEM((blk * nq, 2 * seq * kv), BF16),
                pltpu.VMEM(x_in.shape, BF16),
                pltpu.VMEM(w_o.shape, BF16), pltpu.VMEM((nc, 128, hd), F32), pltpu.VMEM((2 * nc, 1, 128), F32),
                pltpu.VMEM((nc, hd // 128, 64, 128), F32), pltpu.VMEM((nc, 1, 128), F32),
                pltpu.VMEM((nc, hd // 128, 64, 128), F32), pltpu.VMEM((nc, 1, 128), F32),
                pltpu.VMEM((nc, hd // 128, 64, 128), F32), pltpu.VMEM((nc, 1, 128), F32),
                pltpu.VMEM((2, 128, 128), F32), pltpu.VMEM((hd // 128, 128, 128), F32),
                pltpu.VMEM((nc,) + d_f32, F32), pltpu.VMEM((nc,) + d_f32, F32), pltpu.VMEM((nc,) + d_f32, F32),
                pltpu.VMEM((8 * nc,) + d_f32, F32),
                dma((2,)), dma((2, late // blk))] + [dma((nc,))] * 18,
            compiler_params=pltpu.CompilerParams(vmem_limit_bytes=24_000_000, collective_id=0, has_side_effects=True),
            cost_estimate=pl.CostEstimate(flops=10 ** 10, bytes_accessed=100_000_000, transcendentals=0),
        )(cur_pos, o_part, lse, q_c, ke_c, ve_c, x_in, w_post, w_o, k_cache, v_cache)
        x_out, k_out, v_out, _ = pl.pallas_call(
            functools.partial(close_kernel, (early, blk, seq, nq, kv)),
            name='close',
            out_shape=[jax.ShapeDtypeStruct(x_in.shape, BF16), jax.ShapeDtypeStruct(k_cache.shape, BF16),
                       jax.ShapeDtypeStruct(v_cache.shape, BF16), late_shape],
            in_specs=[smem] + [vmem] * 4 + [hbm, hbm],
            out_specs=[hbm, hbm, hbm, vmem],
            input_output_aliases={4: 3, 5: 1, 6: 2},
            scratch_shapes=[dma, dma((2, late // blk))],
            compiler_params=pltpu.CompilerParams(vmem_limit_bytes=4_000_000),
        )(cur_pos, x_new, ke_c, ve_c, kv_late, k_part, v_part)
        return x_out, k_out, v_out

    return jax.shard_map(local_step, mesh=mesh,
                         in_specs=(P('dp', None), P('dp'), P(None), P(None, 'tp'), P(None, 'tp'), P(None, 'tp'), P('tp', None), P(None), cache_spec, cache_spec),
                         out_specs=(P('dp', None), cache_spec, cache_spec), check_vma=False)
```
